512 devices in a mesh: sta: 32 (over z_lo, y), seg: 16 (over z_hi, x, core).
Axes of the slice: x: 4, y: 4, z: 16 (z_hi: 2, z_lo: 8; z = z_hi * 8 + z_lo), core: 2. Of those that a mesh axis runs over, the one named last changes fastest.
Arguments:
- spectra: bfloat16 [192, 64, 2, 1024], P('sta', 'seg'), may hold values from -6 to 6
- observed: float32 [544, 6, 6, 512], P('sta'), may hold values from -8 to 8
- pair_table: int32 [544, 2], P('sta'), may hold values from -1 to 31, as said below
Outputs:
- gradient: float32 [192, 2, 1024], P('sta', None, 'seg')
The draws below stay inside these ranges and needn't reach their ends.
Inputs may be any that keep to these rules, and one draw needn't show every extreme that they name: `pair_table`: rows are slots; each unordered pair of station blocks p <= q of the 32 blocks stands in exactly one row as (p, q); every other row is (-1, -1).
All inputs are finite; a program needn't handle non-finite values.
Results may differ from the reference program's by a relative error of at most 0.0013.
Values may be sent and summed in bfloat16 or wider, within the bound.
A program may use at most 64 MiB of HBM per device.

```python
import math
import jax
import jax.numpy as jnp
import numpy as np
from jax import lax

STA_DEV = 6
SEG_DEV = 4
F = 1024
LAGS = 512
STATIONS = 192
SEGS = 64
BLOCKS = 32
SLOTS = 544


def draw_pair_table(key, part):
    upper_first, upper_second = np.triu_indices(BLOCKS)
    block_pairs = jnp.stack([jnp.asarray(upper_first, jnp.int32), jnp.asarray(upper_second, jnp.int32)], axis=1)
    filler = -jnp.ones((SLOTS - block_pairs.shape[0], 2), jnp.int32)
    slot_rows = jnp.concatenate([block_pairs, filler], axis=0)
    shuffle_order = jax.random.permutation(jax.random.fold_in(key, 11), SLOTS)
    return slot_rows[shuffle_order]


def level_of(key, dims, cuts, smallest, top_value):
    loudness = 1.0
    for axis_at, blocks in cuts:
        steps = jax.random.uniform(jax.random.fold_in(jax.random.fold_in(key, 6), axis_at), (blocks,), jnp.float32, smallest / len(cuts), top_value / len(cuts))
        loudness = loudness * jnp.repeat(jnp.exp(steps), dims[axis_at] // blocks).reshape((-1,) + (1,) * (len(dims) - 1 - axis_at))
    return loudness


def bell_draw(rng, shape, spread, limit, shards=(), kind=jnp.bfloat16):
    factor_of = level_of(rng, shape, shards, -0.22, 0.18) if shards else 1.0
    array = jax.random.normal(rng, shape, jnp.float32) * spread * factor_of
    return jnp.minimum(jnp.maximum(array, -limit), limit).astype(kind)


def setup_inputs(seed: int = 0) -> dict:
    seeds = jax.random.split(jax.random.key(seed), 4)
    spectra = bell_draw(seeds[0], (STATIONS, SEGS, 2, F), 1.0, 6.0, ((0, 32), (1, 16)))
    observed = bell_draw(seeds[1], (SLOTS, STA_DEV, STA_DEV, LAGS), 1.5, 8.0, ((0, 32),), jnp.float32)
    pair_table = draw_pair_table(jax.random.fold_in(seeds[3], 71), 0)
    return dict(spectra=spectra, observed=observed, pair_table=pair_table)


def lag_kernel(start, count):
    frequency = (start + jnp.arange(count, dtype=jnp.int32))[:, None]
    offset = jnp.arange(LAGS, dtype=jnp.int32)[None, :] - LAGS // 2
    phase = jnp.mod(frequency * offset, 2 * F)
    angle = math.pi / F * phase.astype(jnp.float32)
    return jnp.stack([jnp.cos(angle), -jnp.sin(angle)], axis=0).astype(jnp.bfloat16)

def group_cross(left, right, groups):
    station_count = left.shape[0]
    left = left.reshape(station_count, groups, -1, 2, left.shape[-1]).astype(jnp.float32)
    right = right.reshape(station_count, groups, -1, 2, right.shape[-1]).astype(jnp.float32)
    left_real = left[:, :, :, 0][:, None]
    left_imag = left[:, :, :, 1][:, None]
    right_real = right[:, :, :, 0][None]
    right_imag = right[:, :, :, 1][None]
    cross_real = lax.optimization_barrier(jnp.sum(left_real * right_real + left_imag * right_imag, axis=3))
    cross_imag = lax.optimization_barrier(jnp.sum(left_imag * right_real - left_real * right_imag, axis=3))
    return jnp.stack([cross_real, cross_imag], axis=3).astype(jnp.bfloat16)

def pair_mask(first, second, station_count):
    row_index = jnp.arange(station_count)[:, None]
    col_index = jnp.arange(station_count)[None, :]
    keep = (first >= 0)[..., None, None] & ((first != second)[..., None, None] | (row_index < col_index))
    return keep.astype(jnp.float32)

def adjoint_terms(gamma, stacked):
    gamma_real = gamma[..., 0, :]
    gamma_imag = gamma[..., 1, :]
    stack_real = stacked[..., 0, :]
    stack_imag = stacked[..., 1, :]
    common = gamma_real * stack_real + gamma_imag * stack_imag
    twist = gamma_imag * stack_real - gamma_real * stack_imag
    left_term = jnp.stack([common.sum(-2), twist.sum(-2)], axis=-2)
    right_term = jnp.stack([common.sum(-3), -twist.sum(-3)], axis=-2)
    return (left_term, right_term)

def reference(spectra, observed, pair_table):
    kernel = lag_kernel(jnp.int32(0), F)
    exact = lax.optimization_barrier(kernel).astype(jnp.float32).reshape(2 * F, LAGS)
    scale = 1.0 / math.sqrt(F * SEGS)
    groups = SEGS // SEG_DEV

    def visit(buffer, slot):
        first, second, observe = slot
        start_left = (jnp.maximum(first, 0) * STA_DEV).astype(jnp.int32)
        start_right = (jnp.maximum(second, 0) * STA_DEV).astype(jnp.int32)
        left = lax.dynamic_slice_in_dim(spectra, start_left, STA_DEV, 0)
        right = lax.dynamic_slice_in_dim(spectra, start_right, STA_DEV, 0)
        crossed = group_cross(left, right, groups)
        stacked = lax.optimization_barrier(jnp.sum(lax.optimization_barrier(crossed).astype(jnp.float32), axis=2))
        lags = scale * jnp.dot(stacked.reshape(-1, 2 * F), exact, precision=lax.Precision.HIGHEST)
        keep = pair_mask(first, second, STA_DEV).reshape(-1, 1)
        residual = (keep * jnp.tanh(lags - observe.reshape(-1, LAGS))).astype(jnp.bfloat16)
        gamma = scale * jnp.dot(residual.astype(jnp.float32), exact.T, precision=lax.Precision.HIGHEST)
        gamma = gamma.reshape(STA_DEV, STA_DEV, 2, F)
        left_term, right_term = adjoint_terms(gamma, stacked)
        current = lax.dynamic_slice_in_dim(buffer, start_left, STA_DEV, 0)
        buffer = lax.dynamic_update_slice_in_dim(buffer, current + left_term, start_left, 0)
        current = lax.dynamic_slice_in_dim(buffer, start_right, STA_DEV, 0)
        buffer = lax.dynamic_update_slice_in_dim(buffer, current + right_term, start_right, 0)
        return (buffer, None)
    buffer = jnp.zeros((STATIONS, 2, F), jnp.float32)
    result, _ = lax.scan(visit, buffer, (pair_table[:, 0], pair_table[:, 1], observed))
    return result
```

```python
import math

import jax
import jax.numpy as jnp
from jax import lax
from jax.experimental import pallas as pl
from jax.experimental.pallas import tpu as pltpu
from jax.sharding import Mesh
from jax.sharding import PartitionSpec as P

F = 1024
LAGS = 512
STA_DEV = 6
SEGS = 64
SEG = ("seg_0", "seg_1", "seg_2")
STA = ("sta_0", "sta_1")
SCALE = 1.0 / math.sqrt(F * SEGS)
NEAR = 8
FAR = 64
F32 = jnp.float32
BF16 = jnp.bfloat16
NT = (((1,), (1,)), ((), ()))


def lag_kernel():
    frequency = jnp.arange(F, dtype=jnp.int32)[:, None]
    offset = jnp.arange(LAGS, dtype=jnp.int32)[None, :] - LAGS // 2
    phase = jnp.mod(frequency * offset, 2 * F)
    angle = math.pi / F * phase.astype(F32)
    kernel = jnp.stack([jnp.cos(angle), -jnp.sin(angle)], axis=0).astype(BF16)
    kernel = kernel.reshape(2, 2, 4, 2, 64, LAGS).transpose(3, 0, 2, 1, 4, 5)
    return kernel.reshape(4, 512, LAGS)


def far_id(index):
    return {"seg_0": index // 32, "sta_0": (index // 4) % 8, "sta_1": index % 4}


def near_id(index):
    return {"seg_1": index // 2, "seg_2": index % 2}


def exchange(count, me, device_of, source, target, send_sems, recv_sems):
    def copy_to(peer):
        return pltpu.make_async_remote_copy(
            src_ref=source(peer),
            dst_ref=target(me),
            send_sem=send_sems.at[peer],
            recv_sem=recv_sems.at[me],
            device_id=device_of(peer),
            device_id_type=pl.DeviceIdType.MESH,
        )

    def arrival_of(peer):
        return pltpu.make_async_remote_copy(
            src_ref=source(peer),
            dst_ref=target(peer),
            send_sem=send_sems.at[peer],
            recv_sem=recv_sems.at[peer],
            device_id=device_of(peer),
            device_id_type=pl.DeviceIdType.MESH,
        )

    def each(action):
        def step(i, carry):
            action(lax.rem(me + i, count))
            return carry

        lax.fori_loop(1, count, step, 0)

    each(lambda peer: copy_to(peer).start())
    return (
        lambda: each(lambda peer: arrival_of(peer).wait_recv()),
        lambda: each(lambda peer: copy_to(peer).wait_send()),
    )


def lane_iota(shape):
    return lax.broadcasted_iota(jnp.int32, shape, len(shape) - 1)


def body(
    x_ref, table_ref, pairs_ref, observed_ref, kernel_ref, out_ref,
    recv_a, send_b, recv_c, stage_b, stage_g, gram_m, onehot,
    stage_f, send_f, recv_f, send_g, recv_g, s_ref, send_i, recv_i, send_k, recv_k,
    obs_v, kern_v, local_sems, near_sems, far_sems,
):
    zh = lax.axis_index("seg_0")
    far = zh * 32 + lax.axis_index("sta_0") * 4 + lax.axis_index("sta_1")
    near = lax.axis_index("seg_1") * 2 + lax.axis_index("seg_2")
    seg = zh * 8 + near

    loads = [
        pltpu.make_async_copy(observed_ref.at[seg], obs_v.at[pl.ds(0, 6)], local_sems.at[0]),
        pltpu.make_async_copy(
            observed_ref.at[16, jnp.minimum(near, 5)], obs_v.at[6], local_sems.at[1]
        ),
        pltpu.make_async_copy(kernel_ref, kern_v, local_sems.at[2]),
    ]
    for load in loads:
        load.start()

    barrier = pltpu.get_barrier_semaphore()

    def greet(count, me, device_of):
        def step(i, carry):
            pl.semaphore_signal(
                barrier, inc=1, device_id=device_of(lax.rem(me + i, count)),
                device_id_type=pl.DeviceIdType.MESH,
            )
            return carry

        lax.fori_loop(1, count, step, 0)

    greet(FAR, far, far_id)
    greet(NEAR, near, near_id)
    pl.semaphore_wait(barrier, FAR + NEAR - 2)

    wait_a, sent_a = exchange(
        NEAR, near, near_id,
        lambda peer: x_ref.at[:, pl.ds(pl.multiple_of(peer * 128, 128), 128)],
        lambda peer: recv_a.at[peer],
        near_sems.at[0], near_sems.at[1],
    )
    recv_a[near] = x_ref[:, pl.ds(pl.multiple_of(near * 128, 128), 128)]
    stage_b[pl.ds(6, FAR, stride=8), :] = jnp.broadcast_to(table_ref[0:1, :], (FAR, 128))
    stage_b[pl.ds(7, FAR, stride=8), :] = jnp.broadcast_to(table_ref[1:2, :], (FAR, 128))
    wait_a()

    for pair in range(3):
        rows = []
        for a in (2 * pair, 2 * pair + 1):
            for m in range(NEAR):
                rows.append(recv_a[m].astype(F32)[8 * a : 8 * a + 8])
        turned = jnp.concatenate(rows, axis=0).T
        for fi in range(2):
            stage_b[pl.ds(3 * fi + pair, FAR, stride=8), :] = turned[64 * fi : 64 * fi + 64]
    send_b[...] = stage_b[...].reshape(FAR, 8, 128).astype(BF16)
    wait_c, sent_c = exchange(
        FAR, far, far_id,
        lambda peer: send_b.at[peer], lambda peer: recv_c.at[peer],
        far_sems.at[0], far_sems.at[1],
    )
    recv_c[far] = send_b[far]
    wait_c()
    stage_b[...] = recv_c[...].astype(F32).reshape(FAR * 8, 128)

    lane32 = lane_iota((32, 128))
    for fi in range(2):
        stations = []
        for pair in range(3):
            both = stage_b[pl.ds(3 * fi + pair, FAR, stride=8), :]
            low, high = both[0:32], both[32:64]
            stations.append(jnp.where(lane32 < 64, low, pltpu.roll(high, 64, 1)))
            stations.append(jnp.where(lane32 < 64, pltpu.roll(low, 64, 1), high))
        stations += [jnp.zeros((32, 128), F32)] * 2
        plain = jnp.concatenate(stations, axis=0)
        even = lax.rem(lane_iota((256, 128)), 2) == 0
        turned = jnp.where(even, pltpu.roll(plain, 127, 1), -pltpu.roll(plain, 1, 1))
        right = plain.astype(BF16)
        for c, left in enumerate((right, turned.astype(BF16))):
            gram = lax.dot_general(right, left, NT, preferred_element_type=F32)
            at = 256 * (2 * fi + c)
            stage_g[0, at : at + 256, :] = gram[:, 0:128]
            stage_g[1, at : at + 256, :] = gram[:, 128:256]

    for a in range(STA_DEV):
        for tile in range(8):
            kept = None
            for i in range(4):
                piece = stage_g[a // 4, pl.ds(4 * tile + i, 32, stride=32), :]
                shift = 32 * ((i - a) % 4)
                piece = pltpu.roll(piece, shift, 1) if shift else piece
                kept = piece if kept is None else jnp.where(lane32 >= 32 * i, piece, kept)
            gram_m[32 * a : 32 * a + 32, 128 * tile : 128 * tile + 128] = kept.astype(BF16)
    gram_m[192:256, :] = jnp.zeros((64, 1024), BF16)

    first = stage_b[pl.ds(6, FAR, stride=8), :]
    second = stage_b[pl.ds(7, FAR, stride=8), :]
    key = (second * 32.0 + first).astype(jnp.int32)
    row64 = lax.broadcasted_iota(jnp.int32, (FAR, 128), 0)
    main_key = jnp.where(row64 < 32, key, pltpu.roll(key, 120, 1))
    rest_key = jnp.where(row64 < 32, key, -1)
    lane1024 = lane_iota((FAR, 1024))
    for m in range(NEAR + 1):
        column = rest_key[:, 16:17] if m == NEAR else main_key[:, m : m + 1]
        hit = jnp.where(lane1024 == column, 1.0, 0.0)
        onehot[64 * m : 64 * m + 64, :] = hit.astype(BF16)
    slots = lax.dot_general(onehot[...], gram_m[...], NT, preferred_element_type=F32)
    lane64 = lane_iota((FAR, 128))
    for m in range(NEAR):
        stage_f[pl.ds(m, FAR, stride=16), :] = slots[64 * m : 64 * m + 64, 0:128]
        upper = slots[64 * m : 64 * m + 64, 128:256]
        if m < STA_DEV:
            rest = slots[512:576, 128 * (m // 4) : 128 * (m // 4) + 128]
            shift = (64 - 32 * (m % 4)) % 128
            rest = pltpu.roll(rest, shift, 1) if shift else rest
            upper = jnp.where(lane64 < 64, upper, jnp.where(lane64 < 96, rest, 0.0))
        stage_f[pl.ds(8 + m, FAR, stride=16), :] = upper
    send_f[...] = stage_f[...].astype(BF16)

    def chunk16(ref):
        return lambda peer: ref.at[pl.ds(pl.multiple_of(peer * 16, 16), 16), :]

    wait_f, sent_f = exchange(
        FAR, far, far_id, chunk16(send_f), chunk16(recv_f), far_sems.at[2], far_sems.at[3]
    )
    own = pl.ds(pl.multiple_of(far * 16, 16), 16)
    recv_f[own, :] = send_f[own, :]
    wait_f()
    stage_f[...] = recv_f[...].astype(F32)
    for m in range(NEAR):
        for t in range(2):
            part = stage_f[pl.ds(8 * t + m, FAR, stride=16), :]
            send_g[m, :, 128 * t : 128 * t + 128] = part.astype(BF16)
    wait_g, sent_g = exchange(
        NEAR, near, near_id,
        lambda peer: send_g.at[peer], lambda peer: recv_g.at[peer],
        near_sems.at[2], near_sems.at[3],
    )
    recv_g[near] = send_g[near]
    wait_g()

    for xt in range(4):
        low = recv_g[xt].astype(F32)
        high = recv_g[4 + xt].astype(F32)
        for t in range(2):
            square = jnp.concatenate(
                [low[:, 128 * t : 128 * t + 128], high[:, 128 * t : 128 * t + 128]], axis=0
            ).T
            for part in range(4 if t == 0 else 3):
                a = 4 * t + part
                for fc in range(4):
                    at = 32 * part + 8 * fc
                    s_ref[fc, 8 * a : 8 * a + 8, 128 * xt : 128 * xt + 128] = square[at : at + 8]
    for load in loads:
        load.wait()
    lags = jnp.zeros((56, LAGS), F32)
    for fc in range(4):
        lags = lags + jnp.dot(s_ref[fc].astype(BF16), kern_v[fc], preferred_element_type=F32)
    b_index = lax.broadcasted_iota(jnp.int32, (STA_DEV, LAGS), 0)
    rows = []
    for a in range(7):
        slot = seg if a < 6 else 16
        p, q = pairs_ref[slot, 0], pairs_ref[slot, 1]
        floor = jnp.where(p < 0, 99, jnp.where(p != q, -1, a if a < 6 else near))
        if a == 6:
            floor = jnp.where((zh == 0) & (near < 6), floor, 99)
        value = jnp.tanh(SCALE * lags[8 * a : 8 * a + 6] - obs_v[a])
        value = jnp.where(b_index > floor, value, 0.0)
        rows += [value, jnp.zeros((2, LAGS), F32)]
    residual = jnp.concatenate(rows, axis=0).astype(BF16)

    for fi in range(2):
        gamma = [
            SCALE * lax.dot_general(residual, kern_v[2 * fi + c], NT, preferred_element_type=F32)
            for c in range(2)
        ]
        s0, s1 = s_ref[2 * fi], s_ref[2 * fi + 1]
        common = gamma[0] * s0 + gamma[1] * s1
        twist = gamma[1] * s0 - gamma[0] * s1
        for ct, term in enumerate((common, twist)):
            left = [jnp.sum(term[8 * a : 8 * a + 8], axis=0, keepdims=True) for a in range(7)]
            left = jnp.concatenate(left + [jnp.zeros((1, 512), F32)], axis=0)
            right = term[0:8]
            for a in range(1, 6):
                right = right + term[8 * a : 8 * a + 8]
            for i, block in enumerate((left, right, term[48:56])):
                at = 24 * ct + 8 * i
                for xt in range(4):
                    send_i[2 * xt + fi, at : at + 8, :] = block[:, 128 * xt : 128 * xt + 128]
    wait_i, sent_i = exchange(
        NEAR, near, near_id,
        lambda peer: send_i.at[peer], lambda peer: recv_i.at[peer],
        near_sems.at[4], near_sems.at[5],
    )
    recv_i[near] = send_i[near]

    lane = lane_iota((1, 192))
    target = jnp.full((1, 192), -1, jnp.int32)
    sign = jnp.full((1, 192), 1.0, F32)
    rest_p = jnp.where(zh == 0, pairs_ref[16, 0], -1) * 8
    rest_q = jnp.where(zh == 0, pairs_ref[16, 1], -1) * 8
    for m in range(NEAR):
        t = lane - 24 * m
        p = pairs_ref[zh * 8 + m, 0] * 8
        q = pairs_ref[zh * 8 + m, 1] * 8
        value = jnp.where(t < 6, p + t, -1)
        value = jnp.where((t >= 8) & (t < 14), q + t - 8, value)
        if m < 6:
            value = jnp.where(t == 6, rest_p + m, value)
            value = jnp.where((t >= 16) & (t < 22), rest_q + t - 16, value)
        inside = (t >= 0) & (t < 24)
        target = jnp.where(inside, value, target)
        sign = jnp.where(inside & (t >= 8), -1.0, sign)
    match = lax.broadcasted_iota(jnp.int32, (256, 192), 0) == target
    choose = (jnp.where(match, 1.0, 0.0), jnp.where(match, sign, 0.0))
    wait_i()
    sums = []
    for ct in range(2):
        terms = recv_i[:, 24 * ct : 24 * ct + 24, :].reshape(192, 128)
        sums.append(
            jnp.dot(
                choose[ct], terms, precision=lax.Precision.HIGHEST, preferred_element_type=F32
            )
        )
    lane256 = lane_iota((256, 128))
    send_k[0:256, :] = jnp.where(lane256 < 64, sums[0], pltpu.roll(sums[1], 64, 1))
    send_k[256:512, :] = jnp.where(lane256 < 64, pltpu.roll(sums[0], 64, 1), sums[1])

    def chunk8(ref):
        return lambda peer: ref.at[pl.ds(pl.multiple_of(peer * 8, 8), 8), :]

    wait_k, sent_k = exchange(
        FAR, far, far_id, chunk8(send_k), chunk8(recv_k), far_sems.at[4], far_sems.at[5]
    )
    own = pl.ds(pl.multiple_of(far * 8, 8), 8)
    recv_k[own, :] = send_k[own, :]
    wait_k()
    total = recv_k[0:8, :]
    for k in range(1, FAR):
        total = total + recv_k[8 * k : 8 * k + 8, :]
    out_ref[...] = total
    for sent in (sent_a, sent_c, sent_f, sent_g, sent_i, sent_k):
        sent()


def on_device(spectra, observed, pair_table):
    table = jnp.pad(pair_table.T.astype(F32), ((0, 0), (0, 111)))
    vmem = pl.BlockSpec(memory_space=pltpu.VMEM)
    hbm = pl.BlockSpec(memory_space=pl.ANY)
    out = pl.pallas_call(
        body,
        out_shape=jax.ShapeDtypeStruct((8, 128), F32),
        in_specs=[vmem, vmem, pl.BlockSpec(memory_space=pltpu.SMEM), hbm, hbm],
        out_specs=vmem,
        scratch_shapes=[
            pltpu.VMEM((8, 48, 128), BF16),
            pltpu.VMEM((64, 8, 128), BF16),
            pltpu.VMEM((64, 8, 128), BF16),
            pltpu.VMEM((512, 128), F32),
            pltpu.VMEM((2, 1024, 128), F32),
            pltpu.VMEM((256, 1024), BF16),
            pltpu.VMEM((576, 1024), BF16),
            pltpu.VMEM((1024, 128), F32),
            pltpu.VMEM((1024, 128), BF16),
            pltpu.VMEM((1024, 128), BF16),
            pltpu.VMEM((8, 64, 256), BF16),
            pltpu.VMEM((8, 64, 256), BF16),
            pltpu.VMEM((4, 56, 512), F32),
            pltpu.VMEM((8, 48, 128), F32),
            pltpu.VMEM((8, 48, 128), F32),
            pltpu.VMEM((512, 128), F32),
            pltpu.VMEM((512, 128), F32),
            pltpu.VMEM((7, 6, 512), F32),
            pltpu.VMEM((4, 512, 512), BF16),
            pltpu.SemaphoreType.DMA((3,)),
            pltpu.SemaphoreType.DMA((6, NEAR)),
            pltpu.SemaphoreType.DMA((6, FAR)),
        ],
        compiler_params=pltpu.CompilerParams(collective_id=0, has_side_effects=True),
    )(spectra.reshape(48, F), table, pair_table, observed, lag_kernel())
    return out[:STA_DEV].reshape(STA_DEV, 2, 64)


def solution(mesh):
    torus = Mesh(mesh.devices.reshape(8, 4, 2, 4, 2), ("sta_0", "sta_1", "seg_0", "seg_1", "seg_2"))
    in_specs = (P(STA, SEG, None, None), P(STA, None, None, None), P(STA, None))
    out_specs = P(STA, None, SEG)
    return jax.shard_map(
        on_device, mesh=torus, in_specs=in_specs, out_specs=out_specs, check_vma=False
    )
```

```python
import math

import jax
import jax.numpy as jnp
import numpy as np
from jax import lax
from jax.experimental import pallas as pl
from jax.experimental.pallas import tpu as pltpu
from jax.sharding import Mesh
from jax.sharding import PartitionSpec as P

F = 1024
LAGS = 512
STA_DEV = 6
SEGS = 64
SEG = ("seg_0", "seg_1", "seg_2")
STA = ("sta_0", "sta_1")
SCALE = 1.0 / math.sqrt(F * SEGS)
NEAR = 8
FAR = 64
F32 = jnp.float32
BF16 = jnp.bfloat16
NT = (((1,), (1,)), ((), ()))


def lag_kernel():
    frequency = np.arange(F, dtype=np.int32)[:, None]
    offset = np.arange(LAGS, dtype=np.int32)[None, :] - LAGS // 2
    phase = np.mod(frequency * offset, 2 * F)
    angle = np.float32(math.pi / F) * phase.astype(np.float32)
    kernel = np.stack([np.cos(angle), -np.sin(angle)], axis=0)
    kernel = kernel.reshape(2, 2, 4, 2, 64, LAGS).transpose(3, 0, 2, 1, 4, 5)
    return jnp.asarray(kernel.reshape(4, 512, LAGS).astype(BF16))


def lane_maps():
    maps = np.zeros((8, 256, 128), np.float32)
    for a in range(STA_DEV):
        for b in range(STA_DEV):
            pair = STA_DEV * a + b
            for fc in range(4):
                row = 32 * a + 8 * fc + b
                if pair < 32:
                    maps[0, row, 32 * fc + pair] = 1
                    h, i, j = pair // 16, pair // 4 % 4, pair % 4
                    maps[5 + h, row, 32 * i + 8 * fc + 4 + j] = 1
                else:
                    for i in range(4):
                        maps[1 + i, row, 32 * i + 8 * fc + pair - 32] = 1
                    maps[7, row, 8 * fc + 4 + pair - 32] = 1
    return jnp.asarray(maps.astype(BF16))


def thirds(value):
    first = value.astype(BF16)
    rest = value - first.astype(F32)
    second = rest.astype(BF16)
    return first, second, (rest - second.astype(F32)).astype(BF16)


def sixths(index):
    return sum((index >= 6 * i).astype(jnp.int32) for i in range(1, 6))


def far_id(index):
    return {"seg_0": index // 32, "sta_0": (index // 4) % 8, "sta_1": index % 4}


def near_id(index):
    return {"seg_1": index // 2, "seg_2": index % 2}


def exchange(count, me, device_of, source, target, send_sems, recv_sems):
    def copy_to(peer):
        return pltpu.make_async_remote_copy(
            src_ref=source(peer),
            dst_ref=target(me),
            send_sem=send_sems.at[peer],
            recv_sem=recv_sems.at[me],
            device_id=device_of(peer),
            device_id_type=pl.DeviceIdType.MESH,
        )

    def arrival_of(peer):
        return pltpu.make_async_remote_copy(
            src_ref=source(peer),
            dst_ref=target(peer),
            send_sem=send_sems.at[peer],
            recv_sem=recv_sems.at[peer],
            device_id=device_of(peer),
            device_id_type=pl.DeviceIdType.MESH,
        )

    def each(action):
        def step(i, carry):
            if count == FAR:
                i = count - i
                j = i // 4
                dz = (j + 1) // 2 * (1 - 2 * ((j + 1) % 2))
                peer = lax.rem(me // 4 + dz + 16, 16) * 4 + lax.rem(me + i, 4)
            else:
                peer = lax.rem(me + i, count)
            action(peer)
            return carry

        lax.fori_loop(1, count, step, 0)

    each(lambda peer: copy_to(peer).start())
    return (
        lambda: each(lambda peer: arrival_of(peer).wait_recv()),
        lambda: each(lambda peer: copy_to(peer).wait_send()),
    )


def lane_iota(shape):
    return lax.broadcasted_iota(jnp.int32, shape, len(shape) - 1)


def body(
    x_hbm, pairs_hbm, observed_ref, kernel_ref, maps_ref, out_ref,
    x_raw, x_wide, x_ref, recv_a, send_b, recv_c, stage_b, stage_g, gram_m, onehot,
    stage_f, send_f, recv_f, send_g, recv_g, s_ref, send_i, recv_i, send_k, recv_k,
    obs_v, obs_rest, obs_rows, kern_v, maps_v, pairs_ref,
    local_sems, near_sems, far_sems, ring_sems,
):
    zh = lax.axis_index("seg_0")
    far = zh * 32 + lax.axis_index("sta_0") * 4 + lax.axis_index("sta_1")
    near = lax.axis_index("seg_1") * 2 + lax.axis_index("seg_2")
    seg = zh * 8 + near

    load_x = pltpu.make_async_copy(x_hbm, x_raw, local_sems.at[0])
    load_pairs = pltpu.make_async_copy(pairs_hbm, pairs_ref, local_sems.at[1])
    loads = [
        pltpu.make_async_copy(observed_ref.at[seg], obs_v, local_sems.at[2]),
        pltpu.make_async_copy(observed_ref.at[16], obs_rest, local_sems.at[3]),
        pltpu.make_async_copy(kernel_ref, kern_v, local_sems.at[4]),
        pltpu.make_async_copy(maps_ref, maps_v, local_sems.at[5]),
    ]
    barrier = pltpu.get_barrier_semaphore()

    z, y = far // 4, far % 4

    def beside(dz, dy):
        return far_id(lax.rem(z + dz + 16, 16) * 4 + lax.rem(y + dy, 4))

    def greet(semaphore, device):
        pl.semaphore_signal(
            semaphore, inc=1, device_id=device, device_id_type=pl.DeviceIdType.MESH
        )

    for i in range(1, NEAR):
        greet(barrier, near_id(lax.rem(near + i, NEAR)))
    for dy in (1, 2, 3):
        greet(barrier, beside(0, dy))
    for dz in (1, -1):
        greet(barrier, beside(dz, 0))
    load_x.start()
    load_pairs.start()
    for load in loads:
        load.start()
    load_pairs.wait()
    lane = lane_iota((1, 128))
    for end in range(2):
        row = jnp.zeros((1, 128), F32)
        for slot in range(17):
            row = jnp.where(lane == slot, pairs_ref[end, slot].astype(F32), row)
        stage_b[pl.ds(6 + end, FAR, stride=8), :] = jnp.broadcast_to(row, (FAR, 128))
    load_x.wait()
    for i in range(24):
        x_wide[2 * i : 2 * i + 2, :] = x_raw[i // 4, i % 4].astype(F32)
    x_ref[...] = x_wide[...].astype(BF16)
    pl.semaphore_wait(barrier, NEAR - 1 + 5)

    wait_a, sent_a = exchange(
        NEAR, near, near_id,
        lambda peer: x_ref.at[:, pl.ds(pl.multiple_of(peer * 128, 128), 128)],
        lambda peer: recv_a.at[peer],
        near_sems.at[0], near_sems.at[1],
    )
    recv_a[near] = x_ref[:, pl.ds(pl.multiple_of(near * 128, 128), 128)]

    for step, distance in enumerate((1, 2, 4)):
        greet(ring_sems.at[step], beside(distance, 0))
        greet(ring_sems.at[step], beside(-distance, 0))
        pl.semaphore_wait(ring_sems.at[step], 2)
    greet(ring_sems.at[3], beside(-1, 0))
    pl.semaphore_wait(ring_sems.at[3], 1)
    wait_a()

    for pair in range(3):
        rows = []
        for a in (2 * pair, 2 * pair + 1):
            for m in range(NEAR):
                rows.append(recv_a[m].astype(F32)[8 * a : 8 * a + 8])
        turned = jnp.concatenate(rows, axis=0).T
        for fi in range(2):
            stage_b[pl.ds(3 * fi + pair, FAR, stride=8), :] = turned[64 * fi : 64 * fi + 64]
    send_b[...] = stage_b[...].reshape(FAR, 8, 128).astype(BF16)
    wait_c, sent_c = exchange(
        FAR, far, far_id,
        lambda peer: send_b.at[peer], lambda peer: recv_c.at[peer],
        far_sems.at[0], far_sems.at[1],
    )
    recv_c[far] = send_b[far]
    for load in loads:
        load.wait()
    for a in range(STA_DEV):
        obs_rows[6 * a : 6 * a + 6, :] = obs_v[a]
    for j in range(4):
        pair = jnp.minimum(4 * seg + j, 35)
        obs_rows[36 + j : 37 + j, :] = obs_rest[pair // 6, pl.ds(pair % 6, 1), :]
    wait_c()
    stage_b[...] = recv_c[...].astype(F32).reshape(FAR * 8, 128)

    lane32 = lane_iota((32, 128))
    for fi in range(2):
        stations = []
        for pair in range(3):
            both = stage_b[pl.ds(3 * fi + pair, FAR, stride=8), :]
            low, high = both[0:32], both[32:64]
            stations.append(jnp.where(lane32 < 64, low, pltpu.roll(high, 64, 1)))
            stations.append(jnp.where(lane32 < 64, pltpu.roll(low, 64, 1), high))
        stations += [jnp.zeros((32, 128), F32)] * 2
        plain = jnp.concatenate(stations, axis=0)
        even = lax.rem(lane_iota((256, 128)), 2) == 0
        turned = jnp.where(even, pltpu.roll(plain, 127, 1), -pltpu.roll(plain, 1, 1))
        right = plain.astype(BF16)
        for c, left in enumerate((right, turned.astype(BF16))):
            gram = lax.dot_general(right, left, NT, preferred_element_type=F32)
            at = 256 * (2 * fi + c)
            stage_g[0, at : at + 256, :] = gram[:, 0:128]
            stage_g[1, at : at + 256, :] = gram[:, 128:256]

    for a in range(STA_DEV):
        for tile in range(8):
            kept = None
            for i in range(4):
                piece = stage_g[a // 4, pl.ds(4 * tile + i, 32, stride=32), :]
                shift = 32 * ((i - a) % 4)
                piece = pltpu.roll(piece, shift, 1) if shift else piece
                kept = piece if kept is None else jnp.where(lane32 >= 32 * i, piece, kept)
            gram_m[32 * a : 32 * a + 32, 128 * tile : 128 * tile + 128] = kept.astype(BF16)
    gram_m[192:256, :] = jnp.zeros((64, 1024), BF16)

    first = stage_b[pl.ds(6, FAR, stride=8), :]
    second = stage_b[pl.ds(7, FAR, stride=8), :]
    key = (second * 32.0 + first).astype(jnp.int32)
    row64 = lax.broadcasted_iota(jnp.int32, (FAR, 128), 0)
    main_key = jnp.where(row64 < 32, key, pltpu.roll(key, 120, 1))
    lane1024 = lane_iota((FAR, 1024))
    for m in range(NEAR + 1):
        column = key[:, 16:17] if m == NEAR else main_key[:, m : m + 1]
        hit = jnp.where(lane1024 == column, 1.0, 0.0)
        onehot[64 * m : 64 * m + 64, :] = hit.astype(BF16)
    slots = lax.dot_general(onehot[...], gram_m[...], NT, preferred_element_type=F32)
    slots = slots.astype(BF16)
    kept = jnp.dot(slots[0:512], maps_v[0], preferred_element_type=F32)
    for m in range(NEAR):
        stage_f[pl.ds(m, FAR, stride=16), :] = kept[64 * m : 64 * m + 64]
    rest = slots[512:576]
    upper = lax.broadcasted_iota(jnp.int32, (FAR, 256), 0) < 32
    rest_low = jnp.where(upper, rest, jnp.zeros_like(rest))
    rest_high = jnp.where(upper, jnp.zeros_like(rest), rest)
    for h in range(2):
        tail = jnp.dot(rest_low, maps_v[5 + h], preferred_element_type=F32)
        if h == 0:
            tail = tail + jnp.dot(rest_high, maps_v[7], preferred_element_type=F32)
        for i in range(4):
            at = 64 * (4 * h + i)
            tail = tail + jnp.dot(
                slots[at : at + 64], maps_v[1 + i], preferred_element_type=F32
            )
        stage_f[pl.ds(8 + h, FAR, stride=16), :] = tail
    send_f[...] = stage_f[...].astype(BF16)

    def chunk16(ref):
        return lambda peer: ref.at[pl.ds(pl.multiple_of(peer * 16, 16), 10), :]

    wait_f, sent_f = exchange(
        FAR, far, far_id, chunk16(send_f), chunk16(recv_f), far_sems.at[2], far_sems.at[3]
    )
    own = pl.ds(pl.multiple_of(far * 16, 16), 16)
    recv_f[own, :] = send_f[own, :]
    wait_f()
    stage_f[...] = recv_f[...].astype(F32)
    lane16 = lane_iota((16, 128))
    tails = [stage_f[pl.ds(8 + h, FAR, stride=16), :] for h in range(2)]
    for m in range(NEAR):
        send_g[m, 0:64, :] = stage_f[pl.ds(m, FAR, stride=16), :].astype(BF16)
        packed = None
        for i in range(4):
            piece = tails[m // 4][16 * i : 16 * i + 16]
            shift = 32 * ((i - m) % 4)
            piece = pltpu.roll(piece, shift, 1) if shift else piece
            packed = piece if packed is None else jnp.where(lane16 >= 32 * i, piece, packed)
        send_g[m, 64:80, :] = packed.astype(BF16)
    wait_g, sent_g = exchange(
        NEAR, near, near_id,
        lambda peer: send_g.at[peer], lambda peer: recv_g.at[peer],
        near_sems.at[2], near_sems.at[3],
    )
    recv_g[near] = send_g[near]
    wait_g()

    tail_rows = []
    for m in range(NEAR):
        blocks = recv_g[m, 64:80, :].astype(F32)
        for i in range(4):
            shift = 32 * ((m - i) % 4)
            tail_rows.append(pltpu.roll(blocks, shift, 1) if shift else blocks)
    lane128 = lane_iota((128, 128))
    tail = None
    for xt in range(4):
        both = jnp.concatenate(tail_rows[4 * xt : 4 * xt + 4] + tail_rows[4 * xt + 16 : 4 * xt + 20])
        tail = both if tail is None else jnp.where(lane128 >= 32 * xt, both, tail)
    tail = tail.T
    for xt in range(4):
        lanes = slice(128 * xt, 128 * xt + 128)
        square = jnp.concatenate(
            [recv_g[xt, 0:64, :].astype(F32), recv_g[4 + xt, 0:64, :].astype(F32)], axis=0
        ).T
        for fc in range(4):
            s_ref[fc, 0:32, lanes] = square[32 * fc : 32 * fc + 32]
            s_ref[fc, 32:40, lanes] = tail[32 * xt + 8 * fc : 32 * xt + 8 * fc + 8]
    lags = jnp.zeros((40, LAGS), F32)
    for fc in range(4):
        lags = lags + jnp.dot(s_ref[fc].astype(BF16), kern_v[fc], preferred_element_type=F32)

    def floor_of(slot):
        p, q = pairs_ref[0, slot], pairs_ref[1, slot]
        return jnp.where(p < 0, 99, jnp.where(p != q, -99, 0))

    row = lax.broadcasted_iota(jnp.int32, (40, LAGS), 0)
    pair = jnp.where(row < 36, row, jnp.minimum(row - 36 + 4 * seg, 35))
    floor = jnp.where(row < 36, floor_of(seg), jnp.where(seg < 9, floor_of(16), 99))
    keep = pair - 7 * sixths(pair) > floor
    value = jnp.tanh(SCALE * lags - obs_rows[...])
    residual = jnp.where(keep, value, 0.0).astype(BF16)

    to = lax.broadcasted_iota(jnp.int32, (16, 40), 0)
    of = lane_iota((16, 40))
    first_of = sixths(of)
    main = of < 36
    picked = (to < 6) & main & (first_of == to)
    picked = picked | ((to >= 6) & (to < 12) & main & (of - 6 * first_of == to - 6))
    picked = picked | ((of >= 36) & (of - 36 == to - 12))
    picked = jnp.where(picked, 1.0, 0.0).astype(BF16)
    for fi in range(2):
        gamma = [
            SCALE * lax.dot_general(residual, kern_v[2 * fi + c], NT, preferred_element_type=F32)
            for c in range(2)
        ]
        s0, s1 = s_ref[2 * fi], s_ref[2 * fi + 1]
        common = gamma[0] * s0 + gamma[1] * s1
        twist = gamma[1] * s0 - gamma[0] * s1
        for ct, term in enumerate((common, twist)):
            block = sum(
                jnp.dot(picked, third, preferred_element_type=F32) for third in thirds(term)
            )
            for xt in range(4):
                send_i[2 * xt + fi, 16 * ct : 16 * ct + 16, :] = block[:, 128 * xt : 128 * xt + 128]
    wait_i, sent_i = exchange(
        NEAR, near, near_id,
        lambda peer: send_i.at[peer], lambda peer: recv_i.at[peer],
        near_sems.at[4], near_sems.at[5],
    )
    recv_i[near] = send_i[near]

    lane = lane_iota((1, 128))
    source = lax.shift_right_logical(lane, 4)
    t = lane - 16 * source
    p_main = jnp.full((1, 128), -1, jnp.int32)
    q_main = p_main
    for m in range(NEAR):
        p_main = jnp.where(source == m, pairs_ref[0, zh * 8 + m], p_main)
        q_main = jnp.where(source == m, pairs_ref[1, zh * 8 + m], q_main)
    pair = jnp.clip(32 * zh + 4 * source + t - 12, 0, 35)
    valid = 32 * zh + 4 * source + t - 12 < 36
    a_rest = sixths(pair)
    plus = jnp.where(
        t < 6, 8 * p_main + t,
        jnp.where((t >= 12) & valid, 8 * pairs_ref[0, 16] + a_rest, -1),
    )
    minus = jnp.where(
        (t >= 6) & (t < 12), 8 * q_main + t - 6,
        jnp.where((t >= 12) & valid, 8 * pairs_ref[1, 16] + pair - 6 * a_rest, -1),
    )
    station = lax.broadcasted_iota(jnp.int32, (256, 128), 0)
    plus = jnp.where(station == plus, 1.0, 0.0)
    minus = jnp.where(station == minus, 1.0, 0.0)
    choose = ((plus + minus).astype(BF16), (plus - minus).astype(BF16))
    wait_i()
    sums = []
    for ct in range(2):
        terms = recv_i[:, 16 * ct : 16 * ct + 16, :].reshape(128, 128)
        sums.append(
            sum(jnp.dot(choose[ct], third, preferred_element_type=F32) for third in thirds(terms))
        )
    lane256 = lane_iota((256, 128))
    send_k[0:256, :] = jnp.where(lane256 < 64, sums[0], pltpu.roll(sums[1], 64, 1))
    send_k[256:512, :] = jnp.where(lane256 < 64, pltpu.roll(sums[0], 64, 1), sums[1])

    def chunk8(ref):
        return lambda peer: ref.at[pl.ds(pl.multiple_of(peer * 8, 8), STA_DEV), :]

    wait_k, sent_k = exchange(
        FAR, far, far_id, chunk8(send_k), chunk8(recv_k), far_sems.at[4], far_sems.at[5]
    )
    own = pl.ds(pl.multiple_of(far * 8, 8), 8)
    recv_k[own, :] = send_k[own, :]
    wait_k()
    total = recv_k[0:8, :]
    for k in range(1, FAR):
        total = total + recv_k[8 * k : 8 * k + 8, :]
    out_ref[:, 0, :] = total[0:STA_DEV, 0:64]
    out_ref[:, 1, :] = total[0:STA_DEV, 64:128]
    for sent in (sent_a, sent_c, sent_f, sent_g, sent_i, sent_k):
        sent()


def on_device(spectra, observed, pair_table):
    vmem = pl.BlockSpec(memory_space=pltpu.VMEM)
    hbm = pl.BlockSpec(memory_space=pl.ANY)
    return pl.pallas_call(
        body,
        out_shape=jax.ShapeDtypeStruct((STA_DEV, 2, 64), F32),
        in_specs=[hbm] * 5,
        out_specs=vmem,
        scratch_shapes=[
            pltpu.VMEM((6, 4, 2, 1024), BF16),
            pltpu.VMEM((48, 1024), F32),
            pltpu.VMEM((48, 1024), BF16),
            pltpu.VMEM((8, 48, 128), BF16),
            pltpu.VMEM((64, 8, 128), BF16),
            pltpu.VMEM((64, 8, 128), BF16),
            pltpu.VMEM((512, 128), F32),
            pltpu.VMEM((2, 1024, 128), F32),
            pltpu.VMEM((256, 1024), BF16),
            pltpu.VMEM((576, 1024), BF16),
            pltpu.VMEM((1024, 128), F32),
            pltpu.VMEM((1024, 128), BF16),
            pltpu.VMEM((1024, 128), BF16),
            pltpu.VMEM((8, 80, 128), BF16),
            pltpu.VMEM((8, 80, 128), BF16),
            pltpu.VMEM((4, 40, 512), F32),
            pltpu.VMEM((8, 32, 128), F32),
            pltpu.VMEM((8, 32, 128), F32),
            pltpu.VMEM((512, 128), F32),
            pltpu.VMEM((512, 128), F32),
            pltpu.VMEM((6, 6, 512), F32),
            pltpu.VMEM((6, 6, 512), F32),
            pltpu.VMEM((40, 512), F32),
            pltpu.VMEM((4, 512, 512), BF16),
            pltpu.VMEM((8, 256, 128), BF16),
            pltpu.SMEM((2, 17), jnp.int32),
            pltpu.SemaphoreType.DMA((6,)),
            pltpu.SemaphoreType.DMA((6, NEAR)),
            pltpu.SemaphoreType.DMA((6, FAR)),
            pltpu.SemaphoreType.REGULAR((4,)),
        ],
        compiler_params=pltpu.CompilerParams(collective_id=0, has_side_effects=True),
    )(spectra, pair_table.T, observed, lag_kernel(), lane_maps())


def solution(mesh):
    torus = Mesh(mesh.devices.reshape(8, 4, 2, 4, 2), ("sta_0", "sta_1", "seg_0", "seg_1", "seg_2"))
    in_specs = (P(STA, SEG, None, None), P(STA, None, None, None), P(STA, None))
    out_specs = P(STA, None, SEG)
    return jax.shard_map(
        on_device, mesh=torus, in_specs=in_specs, out_specs=out_specs, check_vma=False
    )
```

```python
import math

import jax
import jax.numpy as jnp
import numpy as np
from jax import lax
from jax.experimental import pallas as pl
from jax.experimental.pallas import tpu as pltpu
from jax.sharding import Mesh
from jax.sharding import PartitionSpec as P

F = 1024
LAGS = 512
STA_DEV = 6
SEGS = 64
SEG = ("seg_0", "seg_1", "seg_2")
STA = ("sta_0", "sta_1")
SCALE = 1.0 / math.sqrt(F * SEGS)
NEAR = 8
FAR = 64
F32 = jnp.float32
BF16 = jnp.bfloat16
NT = (((1,), (1,)), ((), ()))


def lag_kernel():
    frequency = np.arange(F, dtype=np.int32)[:, None]
    offset = np.arange(LAGS, dtype=np.int32)[None, :] - LAGS // 2
    phase = np.mod(frequency * offset, 2 * F)
    angle = np.float32(math.pi / F) * phase.astype(np.float32)
    kernel = np.stack([np.cos(angle), -np.sin(angle)], axis=0)
    kernel = kernel.reshape(2, 2, 4, 2, 64, LAGS).transpose(3, 0, 2, 1, 4, 5)
    return jnp.asarray(kernel.reshape(4, 512, LAGS).astype(BF16))


def lane_maps():
    maps = np.zeros((8, 256, 128), np.float32)
    for a in range(STA_DEV):
        for b in range(STA_DEV):
            pair = STA_DEV * a + b
            for fc in range(4):
                row = 32 * a + 8 * fc + b
                if pair < 32:
                    maps[0, row, 32 * fc + pair] = 1
                    h, i, j = pair // 16, pair // 4 % 4, pair % 4
                    maps[5 + h, row, 32 * i + 8 * fc + 4 + j] = 1
                else:
                    for i in range(4):
                        maps[1 + i, row, 32 * i + 8 * fc + pair - 32] = 1
                    maps[7, row, 8 * fc + 4 + pair - 32] = 1
    return jnp.asarray(maps.astype(BF16))


def thirds(value):
    first = value.astype(BF16)
    rest = value - first.astype(F32)
    second = rest.astype(BF16)
    return first, second, (rest - second.astype(F32)).astype(BF16)


def sixths(index):
    return sum((index >= 6 * i).astype(jnp.int32) for i in range(1, 6))


def far_id(index):
    return {"seg_0": index // 32, "sta_0": (index // 4) % 8, "sta_1": index % 4}


def near_id(index):
    return {"seg_1": index // 2, "seg_2": index % 2}


def landed(ref, semaphore):
    pltpu.make_async_copy(ref, ref, semaphore).wait()


def send(source, target, semaphores, at, device):
    pltpu.make_async_remote_copy(
        src_ref=source,
        dst_ref=target,
        send_sem=semaphores.at[at],
        recv_sem=semaphores.at[at + 1],
        device_id=device,
        device_id_type=pl.DeviceIdType.MESH,
    ).start()


def send_near(me, source, target, semaphores, at):
    for i in range(1, NEAR):
        peer = lax.rem(me + i, NEAR)
        send(source(peer), target(me), semaphores, at, near_id(peer))


def send_far(me, source, target, semaphores, at, farthest_first):
    z, y = me // 4, lax.rem(me, 4)
    ys = [lax.rem(y + dy, 4) for dy in range(4)]

    def to_chip(peer_z, dys):
        zh, zl = peer_z // 8, lax.rem(peer_z, 8)
        for dy in dys:
            peer = peer_z * 4 + ys[dy]
            device = {"seg_0": zh, "sta_0": zl, "sta_1": ys[dy]}
            send(source(peer), target(me), semaphores, at, device)

    def step(j, carry):
        if farthest_first:
            j = 16 - j
            dz = (j + 1) // 2 * (1 - 2 * lax.rem(j + 1, 2))
            to_chip(lax.rem(z + dz + 16, 16), range(4))
        else:
            to_chip(lax.rem(z + j, 16), range(4))
        return carry

    lax.fori_loop(1, 16, step, 0)
    to_chip(z, (1, 2, 3))


def lane_iota(shape):
    return lax.broadcasted_iota(jnp.int32, shape, len(shape) - 1)


def body(
    x_hbm, pairs_hbm, observed_ref, kernel_ref, maps_ref, out_ref,
    x_raw, x_wide, x_ref, recv_a, send_b, recv_c, stage_b, stage_g, gram_m, onehot,
    stage_f, send_f, recv_f, send_g, recv_g, s_ref, send_i, recv_i, send_k, recv_k,
    obs_v, obs_rest, obs_rows, kern_v, maps_v, pairs_ref,
    local_sems, sems, ring_sems,
):
    zh = lax.axis_index("seg_0")
    far = zh * 32 + lax.axis_index("sta_0") * 4 + lax.axis_index("sta_1")
    near = lax.axis_index("seg_1") * 2 + lax.axis_index("seg_2")
    seg = zh * 8 + near

    load_x = pltpu.make_async_copy(x_hbm, x_raw, local_sems.at[0])
    load_pairs = pltpu.make_async_copy(pairs_hbm, pairs_ref, local_sems.at[1])
    loads = [
        pltpu.make_async_copy(observed_ref.at[seg], obs_v, local_sems.at[2]),
        pltpu.make_async_copy(observed_ref.at[16], obs_rest, local_sems.at[3]),
        pltpu.make_async_copy(kernel_ref, kern_v, local_sems.at[4]),
        pltpu.make_async_copy(maps_ref, maps_v, local_sems.at[5]),
    ]
    barrier = pltpu.get_barrier_semaphore()

    z, y = far // 4, far % 4

    def beside(dz, dy):
        return far_id(lax.rem(z + dz + 16, 16) * 4 + lax.rem(y + dy, 4))

    def greet(semaphore, device):
        pl.semaphore_signal(
            semaphore, inc=1, device_id=device, device_id_type=pl.DeviceIdType.MESH
        )

    for i in range(1, NEAR):
        greet(barrier, near_id(lax.rem(near + i, NEAR)))
    for dy in (1, 2, 3):
        greet(barrier, beside(0, dy))
    for dz in (1, -1):
        greet(barrier, beside(dz, 0))
    load_x.start()
    load_pairs.start()
    for load in loads:
        load.start()
    load_pairs.wait()
    lane = lane_iota((1, 128))
    for end in range(2):
        row = jnp.zeros((1, 128), F32)
        for slot in range(17):
            row = jnp.where(lane == slot, pairs_ref[end, slot].astype(F32), row)
        stage_b[pl.ds(6 + end, FAR, stride=8), :] = jnp.broadcast_to(row, (FAR, 128))
    load_x.wait()
    for i in range(24):
        x_wide[2 * i : 2 * i + 2, :] = x_raw[i // 4, i % 4].astype(F32)
    x_ref[...] = x_wide[...].astype(BF16)
    pl.semaphore_wait(barrier, NEAR - 1 + 5)

    send_near(
        near,
        lambda peer: x_ref.at[:, pl.ds(pl.multiple_of(peer * 128, 128), 128)],
        lambda peer: recv_a.at[peer],
        sems, 0,
    )
    recv_a[near] = x_ref[:, pl.ds(pl.multiple_of(near * 128, 128), 128)]

    for step, distance in enumerate((1, 2, 4)):
        greet(ring_sems.at[step], beside(distance, 0))
        greet(ring_sems.at[step], beside(-distance, 0))
        pl.semaphore_wait(ring_sems.at[step], 2)
    greet(ring_sems.at[3], beside(-1, 0))
    pl.semaphore_wait(ring_sems.at[3], 1)
    landed(recv_a.at[pl.ds(0, NEAR - 1)], sems.at[1])

    for pair in range(3):
        rows = []
        for a in (2 * pair, 2 * pair + 1):
            for m in range(NEAR):
                rows.append(recv_a[m].astype(F32)[8 * a : 8 * a + 8])
        turned = jnp.concatenate(rows, axis=0).T
        for fi in range(2):
            stage_b[pl.ds(3 * fi + pair, FAR, stride=8), :] = turned[64 * fi : 64 * fi + 64]
    send_b[...] = stage_b[...].reshape(FAR, 8, 128).astype(BF16)
    send_far(far, lambda peer: send_b.at[peer], lambda peer: recv_c.at[peer], sems, 2, False)
    recv_c[far] = send_b[far]
    for load in loads:
        load.wait()
    for a in range(STA_DEV):
        obs_rows[6 * a : 6 * a + 6, :] = obs_v[a]
    for j in range(4):
        pair = jnp.minimum(4 * seg + j, 35)
        obs_rows[36 + j : 37 + j, :] = obs_rest[pair // 6, pl.ds(pair % 6, 1), :]
    landed(recv_a.at[pl.ds(0, NEAR - 1)], sems.at[0])
    landed(recv_c.at[pl.ds(0, FAR - 1)], sems.at[3])
    stage_b[...] = recv_c[...].astype(F32).reshape(FAR * 8, 128)

    lane32 = lane_iota((32, 128))
    for fi in range(2):
        stations = []
        for pair in range(3):
            both = stage_b[pl.ds(3 * fi + pair, FAR, stride=8), :]
            low, high = both[0:32], both[32:64]
            stations.append(jnp.where(lane32 < 64, low, pltpu.roll(high, 64, 1)))
            stations.append(jnp.where(lane32 < 64, pltpu.roll(low, 64, 1), high))
        stations += [jnp.zeros((32, 128), F32)] * 2
        plain = jnp.concatenate(stations, axis=0)
        even = lax.rem(lane_iota((256, 128)), 2) == 0
        turned = jnp.where(even, pltpu.roll(plain, 127, 1), -pltpu.roll(plain, 1, 1))
        right = plain.astype(BF16)
        for c, left in enumerate((right, turned.astype(BF16))):
            gram = lax.dot_general(right, left, NT, preferred_element_type=F32)
            at = 256 * (2 * fi + c)
            stage_g[0, at : at + 256, :] = gram[:, 0:128]
            stage_g[1, at : at + 256, :] = gram[:, 128:256]

    for a in range(STA_DEV):
        for tile in range(8):
            kept = None
            for i in range(4):
                piece = stage_g[a // 4, pl.ds(4 * tile + i, 32, stride=32), :]
                shift = 32 * ((i - a) % 4)
                piece = pltpu.roll(piece, shift, 1) if shift else piece
                kept = piece if kept is None else jnp.where(lane32 >= 32 * i, piece, kept)
            gram_m[32 * a : 32 * a + 32, 128 * tile : 128 * tile + 128] = kept.astype(BF16)
    gram_m[192:256, :] = jnp.zeros((64, 1024), BF16)

    first = stage_b[pl.ds(6, FAR, stride=8), :]
    second = stage_b[pl.ds(7, FAR, stride=8), :]
    key = (second * 32.0 + first).astype(jnp.int32)
    row64 = lax.broadcasted_iota(jnp.int32, (FAR, 128), 0)
    main_key = jnp.where(row64 < 32, key, pltpu.roll(key, 120, 1))
    lane1024 = lane_iota((FAR, 1024))
    for m in range(NEAR + 1):
        column = key[:, 16:17] if m == NEAR else main_key[:, m : m + 1]
        hit = jnp.where(lane1024 == column, 1.0, 0.0)
        onehot[64 * m : 64 * m + 64, :] = hit.astype(BF16)
    slots = lax.dot_general(onehot[...], gram_m[...], NT, preferred_element_type=F32)
    slots = slots.astype(BF16)
    kept = jnp.dot(slots[0:512], maps_v[0], preferred_element_type=F32)
    for m in range(NEAR):
        stage_f[pl.ds(m, FAR, stride=16), :] = kept[64 * m : 64 * m + 64]
    rest = slots[512:576]
    upper = lax.broadcasted_iota(jnp.int32, (FAR, 256), 0) < 32
    rest_low = jnp.where(upper, rest, jnp.zeros_like(rest))
    rest_high = jnp.where(upper, jnp.zeros_like(rest), rest)
    for h in range(2):
        tail = jnp.dot(rest_low, maps_v[5 + h], preferred_element_type=F32)
        if h == 0:
            tail = tail + jnp.dot(rest_high, maps_v[7], preferred_element_type=F32)
        for i in range(4):
            at = 64 * (4 * h + i)
            tail = tail + jnp.dot(
                slots[at : at + 64], maps_v[1 + i], preferred_element_type=F32
            )
        stage_f[pl.ds(8 + h, FAR, stride=16), :] = tail
    send_f[...] = stage_f[...].astype(BF16)

    def chunk16(ref):
        return lambda peer: ref.at[pl.ds(pl.multiple_of(peer * 16, 16), 10), :]

    send_far(far, chunk16(send_f), chunk16(recv_f), sems, 4, True)
    own = pl.ds(pl.multiple_of(far * 16, 16), 16)
    recv_f[own, :] = send_f[own, :]
    landed(send_b.at[pl.ds(0, FAR - 1)], sems.at[2])
    landed(recv_f.at[pl.ds(0, 10 * (FAR - 1))], sems.at[5])
    stage_f[...] = recv_f[...].astype(F32)
    lane16 = lane_iota((16, 128))
    tails = [stage_f[pl.ds(8 + h, FAR, stride=16), :] for h in range(2)]
    for m in range(NEAR):
        send_g[m, 0:64, :] = stage_f[pl.ds(m, FAR, stride=16), :].astype(BF16)
        packed = None
        for i in range(4):
            piece = tails[m // 4][16 * i : 16 * i + 16]
            shift = 32 * ((i - m) % 4)
            piece = pltpu.roll(piece, shift, 1) if shift else piece
            packed = piece if packed is None else jnp.where(lane16 >= 32 * i, piece, packed)
        send_g[m, 64:80, :] = packed.astype(BF16)
    send_near(near, lambda peer: send_g.at[peer], lambda peer: recv_g.at[peer], sems, 6)
    recv_g[near] = send_g[near]
    landed(send_f.at[pl.ds(0, 10 * (FAR - 1))], sems.at[4])
    landed(recv_g.at[pl.ds(0, NEAR - 1)], sems.at[7])

    tail_rows = []
    for m in range(NEAR):
        blocks = recv_g[m, 64:80, :].astype(F32)
        for i in range(4):
            shift = 32 * ((m - i) % 4)
            tail_rows.append(pltpu.roll(blocks, shift, 1) if shift else blocks)
    lane128 = lane_iota((128, 128))
    tail = None
    for xt in range(4):
        both = jnp.concatenate(tail_rows[4 * xt : 4 * xt + 4] + tail_rows[4 * xt + 16 : 4 * xt + 20])
        tail = both if tail is None else jnp.where(lane128 >= 32 * xt, both, tail)
    tail = tail.T
    for xt in range(4):
        lanes = slice(128 * xt, 128 * xt + 128)
        square = jnp.concatenate(
            [recv_g[xt, 0:64, :].astype(F32), recv_g[4 + xt, 0:64, :].astype(F32)], axis=0
        ).T
        for fc in range(4):
            s_ref[fc, 0:32, lanes] = square[32 * fc : 32 * fc + 32]
            s_ref[fc, 32:40, lanes] = tail[32 * xt + 8 * fc : 32 * xt + 8 * fc + 8]
    lags = jnp.zeros((40, LAGS), F32)
    for fc in range(4):
        lags = lags + jnp.dot(s_ref[fc].astype(BF16), kern_v[fc], preferred_element_type=F32)

    def floor_of(slot):
        p, q = pairs_ref[0, slot], pairs_ref[1, slot]
        return jnp.where(p < 0, 99, jnp.where(p != q, -99, 0))

    row = lax.broadcasted_iota(jnp.int32, (40, LAGS), 0)
    pair = jnp.where(row < 36, row, jnp.minimum(row - 36 + 4 * seg, 35))
    floor = jnp.where(row < 36, floor_of(seg), jnp.where(seg < 9, floor_of(16), 99))
    keep = pair - 7 * sixths(pair) > floor
    value = jnp.tanh(SCALE * lags - obs_rows[...])
    residual = jnp.where(keep, value, 0.0).astype(BF16)

    to = lax.broadcasted_iota(jnp.int32, (16, 40), 0)
    of = lane_iota((16, 40))
    first_of = sixths(of)
    main = of < 36
    picked = (to < 6) & main & (first_of == to)
    picked = picked | ((to >= 6) & (to < 12) & main & (of - 6 * first_of == to - 6))
    picked = picked | ((of >= 36) & (of - 36 == to - 12))
    picked = jnp.where(picked, 1.0, 0.0).astype(BF16)
    for fi in range(2):
        gamma = [
            SCALE * lax.dot_general(residual, kern_v[2 * fi + c], NT, preferred_element_type=F32)
            for c in range(2)
        ]
        s0, s1 = s_ref[2 * fi], s_ref[2 * fi + 1]
        common = gamma[0] * s0 + gamma[1] * s1
        twist = gamma[1] * s0 - gamma[0] * s1
        for ct, term in enumerate((common, twist)):
            block = sum(
                jnp.dot(picked, third, preferred_element_type=F32) for third in thirds(term)
            )
            for xt in range(4):
                send_i[2 * xt + fi, 16 * ct : 16 * ct + 16, :] = block[:, 128 * xt : 128 * xt + 128]
    send_near(near, lambda peer: send_i.at[peer], lambda peer: recv_i.at[peer], sems, 8)
    recv_i[near] = send_i[near]

    lane = lane_iota((1, 128))
    source = lax.shift_right_logical(lane, 4)
    t = lane - 16 * source
    p_main = jnp.full((1, 128), -1, jnp.int32)
    q_main = p_main
    for m in range(NEAR):
        p_main = jnp.where(source == m, pairs_ref[0, zh * 8 + m], p_main)
        q_main = jnp.where(source == m, pairs_ref[1, zh * 8 + m], q_main)
    pair = jnp.clip(32 * zh + 4 * source + t - 12, 0, 35)
    valid = 32 * zh + 4 * source + t - 12 < 36
    a_rest = sixths(pair)
    plus = jnp.where(
        t < 6, 8 * p_main + t,
        jnp.where((t >= 12) & valid, 8 * pairs_ref[0, 16] + a_rest, -1),
    )
    minus = jnp.where(
        (t >= 6) & (t < 12), 8 * q_main + t - 6,
        jnp.where((t >= 12) & valid, 8 * pairs_ref[1, 16] + pair - 6 * a_rest, -1),
    )
    station = lax.broadcasted_iota(jnp.int32, (256, 128), 0)
    plus = jnp.where(station == plus, 1.0, 0.0)
    minus = jnp.where(station == minus, 1.0, 0.0)
    choose = ((plus + minus).astype(BF16), (plus - minus).astype(BF16))
    landed(send_g.at[pl.ds(0, NEAR - 1)], sems.at[6])
    landed(recv_i.at[pl.ds(0, NEAR - 1)], sems.at[9])
    sums = []
    for ct in range(2):
        terms = recv_i[:, 16 * ct : 16 * ct + 16, :].reshape(128, 128)
        sums.append(
            sum(jnp.dot(choose[ct], third, preferred_element_type=F32) for third in thirds(terms))
        )
    lane256 = lane_iota((256, 128))
    send_k[0:256, :] = jnp.where(lane256 < 64, sums[0], pltpu.roll(sums[1], 64, 1))
    send_k[256:512, :] = jnp.where(lane256 < 64, pltpu.roll(sums[0], 64, 1), sums[1])

    def chunk8(ref):
        return lambda peer: ref.at[pl.ds(pl.multiple_of(peer * 8, 8), STA_DEV), :]

    send_far(far, chunk8(send_k), chunk8(recv_k), sems, 10, False)
    own = pl.ds(pl.multiple_of(far * 8, 8), 8)
    recv_k[own, :] = send_k[own, :]
    landed(send_i.at[pl.ds(0, NEAR - 1)], sems.at[8])
    landed(recv_k.at[pl.ds(0, STA_DEV * (FAR - 1))], sems.at[11])
    total = recv_k[0:8, :]
    for k in range(1, FAR):
        total = total + recv_k[8 * k : 8 * k + 8, :]
    out_ref[:, 0, :] = total[0:STA_DEV, 0:64]
    out_ref[:, 1, :] = total[0:STA_DEV, 64:128]
    landed(send_k.at[pl.ds(0, STA_DEV * (FAR - 1))], sems.at[10])


def on_device(spectra, observed, pair_table):
    vmem = pl.BlockSpec(memory_space=pltpu.VMEM)
    hbm = pl.BlockSpec(memory_space=pl.ANY)
    return pl.pallas_call(
        body,
        out_shape=jax.ShapeDtypeStruct((STA_DEV, 2, 64), F32),
        in_specs=[hbm] * 5,
        out_specs=vmem,
        scratch_shapes=[
            pltpu.VMEM((6, 4, 2, 1024), BF16),
            pltpu.VMEM((48, 1024), F32),
            pltpu.VMEM((48, 1024), BF16),
            pltpu.VMEM((8, 48, 128), BF16),
            pltpu.VMEM((64, 8, 128), BF16),
            pltpu.VMEM((64, 8, 128), BF16),
            pltpu.VMEM((512, 128), F32),
            pltpu.VMEM((2, 1024, 128), F32),
            pltpu.VMEM((256, 1024), BF16),
            pltpu.VMEM((576, 1024), BF16),
            pltpu.VMEM((1024, 128), F32),
            pltpu.VMEM((1024, 128), BF16),
            pltpu.VMEM((1024, 128), BF16),
            pltpu.VMEM((8, 80, 128), BF16),
            pltpu.VMEM((8, 80, 128), BF16),
            pltpu.VMEM((4, 40, 512), F32),
            pltpu.VMEM((8, 32, 128), F32),
            pltpu.VMEM((8, 32, 128), F32),
            pltpu.VMEM((512, 128), F32),
            pltpu.VMEM((512, 128), F32),
            pltpu.VMEM((6, 6, 512), F32),
            pltpu.VMEM((6, 6, 512), F32),
            pltpu.VMEM((40, 512), F32),
            pltpu.VMEM((4, 512, 512), BF16),
            pltpu.VMEM((8, 256, 128), BF16),
            pltpu.SMEM((2, 17), jnp.int32),
            pltpu.SemaphoreType.DMA((6,)),
            pltpu.SemaphoreType.DMA((12,)),
            pltpu.SemaphoreType.REGULAR((4,)),
        ],
        compiler_params=pltpu.CompilerParams(collective_id=0, has_side_effects=True),
    )(spectra, pair_table.T, observed, lag_kernel(), lane_maps())


def solution(mesh):
    torus = Mesh(mesh.devices.reshape(8, 4, 2, 4, 2), ("sta_0", "sta_1", "seg_0", "seg_1", "seg_2"))
    in_specs = (P(STA, SEG, None, None), P(STA, None, None, None), P(STA, None))
    out_specs = P(STA, None, SEG)
    return jax.shard_map(
        on_device, mesh=torus, in_specs=in_specs, out_specs=out_specs, check_vma=False
    )
```

```python
import math

import jax
import jax.numpy as jnp
import numpy as np
from jax import lax
from jax.experimental import pallas as pl
from jax.experimental.pallas import tpu as pltpu
from jax.sharding import Mesh
from jax.sharding import PartitionSpec as P

F = 1024
LAGS = 512
STA_DEV = 6
SEGS = 64
SEG = ("seg_0", "seg_1", "seg_2")
STA = ("sta_0", "sta_1")
SCALE = 1.0 / math.sqrt(F * SEGS)
NEAR = 8
FAR = 64
F32 = jnp.float32
BF16 = jnp.bfloat16
NT = (((1,), (1,)), ((), ()))


def lag_kernel():
    frequency = np.arange(F, dtype=np.int32)[:, None]
    offset = np.arange(LAGS, dtype=np.int32)[None, :] - LAGS // 2
    phase = np.mod(frequency * offset, 2 * F)
    angle = np.float32(math.pi / F) * phase.astype(np.float32)
    kernel = np.stack([np.cos(angle), -np.sin(angle)], axis=0)
    kernel = kernel.reshape(2, 2, 4, 2, 64, LAGS).transpose(3, 0, 2, 1, 4, 5)
    return jnp.asarray(kernel.reshape(4, 512, LAGS).astype(BF16))


def lane_maps():
    maps = np.zeros((8, 256, 128), np.float32)
    for a in range(STA_DEV):
        for b in range(STA_DEV):
            pair = STA_DEV * a + b
            for fc in range(4):
                row = 32 * a + 8 * fc + b
                if pair < 32:
                    maps[0, row, 32 * fc + pair] = 1
                    h, i, j = pair // 16, pair // 4 % 4, pair % 4
                    maps[5 + h, row, 32 * i + 8 * fc + 4 + j] = 1
                else:
                    for i in range(4):
                        maps[1 + i, row, 32 * i + 8 * fc + pair - 32] = 1
                    maps[7, row, 8 * fc + 4 + pair - 32] = 1
    return jnp.asarray(maps.astype(BF16))


def thirds(value):
    first = value.astype(BF16)
    rest = value - first.astype(F32)
    second = rest.astype(BF16)
    return first, second, (rest - second.astype(F32)).astype(BF16)


def sixths(index):
    return sum((index >= 6 * i).astype(jnp.int32) for i in range(1, 6))


def far_id(index):
    return {"seg_0": index // 32, "sta_0": (index // 4) % 8, "sta_1": index % 4}


def near_id(index):
    return {"seg_1": index // 2, "seg_2": index % 2}


def landed(ref, semaphore):
    pltpu.make_async_copy(ref, ref, semaphore).wait()


def send(source, target, semaphores, at, device):
    pltpu.make_async_remote_copy(
        src_ref=source,
        dst_ref=target,
        send_sem=semaphores.at[at],
        recv_sem=semaphores.at[at + 1],
        device_id=device,
        device_id_type=pl.DeviceIdType.MESH,
    ).start()


def send_near(me, source, target, semaphores, at):
    x, core = me // 2, lax.rem(me, 2)
    for dx, change in ((2, 1), (2, 0), (1, 1), (3, 1), (1, 0), (3, 0), (0, 1)):
        peer = lax.rem(x + dx, 4) * 2 + (1 - core if change else core)
        send(source(peer), target(me), semaphores, at, near_id(peer))


def send_far(me, source, target, semaphores, at, farthest_first):
    z, y = me // 4, lax.rem(me, 4)
    ys = [lax.rem(y + dy, 4) for dy in range(4)]

    def to_chip(peer_z, dys):
        zh, zl = peer_z // 8, lax.rem(peer_z, 8)
        for dy in dys:
            peer = peer_z * 4 + ys[dy]
            device = {"seg_0": zh, "sta_0": zl, "sta_1": ys[dy]}
            send(source(peer), target(me), semaphores, at, device)

    def step(j, carry):
        if farthest_first:
            j = 16 - j
            dz = (j + 1) // 2 * (1 - 2 * lax.rem(j + 1, 2))
            to_chip(lax.rem(z + dz + 16, 16), (2, 1, 3, 0))
        else:
            to_chip(lax.rem(z + j, 16), range(4))
        return carry

    lax.fori_loop(1, 16, step, 0)
    to_chip(z, (2, 1, 3))


def lane_iota(shape):
    return lax.broadcasted_iota(jnp.int32, shape, len(shape) - 1)


def body(
    x_hbm, pairs_hbm, observed_ref, kernel_ref, maps_ref, out_ref,
    x_raw, x_wide, x_ref, recv_a, send_b, recv_c, stage_b, stage_g, gram_m, onehot,
    stage_f, send_f, recv_f, send_g, recv_g, s_ref, send_i, recv_i, send_k, recv_k,
    obs_v, obs_rest, obs_rows, kern_v, maps_v, pairs_ref,
    local_sems, sems, ring_sems,
):
    zh = lax.axis_index("seg_0")
    far = zh * 32 + lax.axis_index("sta_0") * 4 + lax.axis_index("sta_1")
    near = lax.axis_index("seg_1") * 2 + lax.axis_index("seg_2")
    seg = zh * 8 + near

    load_x = pltpu.make_async_copy(x_hbm, x_raw, local_sems.at[0])
    load_pairs = pltpu.make_async_copy(pairs_hbm, pairs_ref, local_sems.at[1])
    loads = [
        pltpu.make_async_copy(observed_ref.at[seg], obs_v, local_sems.at[2]),
        pltpu.make_async_copy(observed_ref.at[16], obs_rest, local_sems.at[3]),
        pltpu.make_async_copy(kernel_ref, kern_v, local_sems.at[4]),
        pltpu.make_async_copy(maps_ref, maps_v, local_sems.at[5]),
    ]
    barrier = pltpu.get_barrier_semaphore()

    z, y = far // 4, far % 4

    def beside(dz, dy):
        return far_id(lax.rem(z + dz + 16, 16) * 4 + lax.rem(y + dy, 4))

    def greet(semaphore, device):
        pl.semaphore_signal(
            semaphore, inc=1, device_id=device, device_id_type=pl.DeviceIdType.MESH
        )

    for i in range(1, NEAR):
        greet(barrier, near_id(lax.rem(near + i, NEAR)))
    for dy in (1, 2, 3):
        greet(barrier, beside(0, dy))
    for dz in (1, -1):
        greet(barrier, beside(dz, 0))
    load_x.start()
    load_pairs.start()
    for load in loads:
        load.start()
    load_pairs.wait()
    lane = lane_iota((1, 128))
    for end in range(2):
        row = jnp.zeros((1, 128), F32)
        for slot in range(17):
            row = jnp.where(lane == slot, pairs_ref[end, slot].astype(F32), row)
        stage_b[pl.ds(6 + end, FAR, stride=8), :] = jnp.broadcast_to(row, (FAR, 128))
    load_x.wait()
    for i in range(24):
        x_wide[2 * i : 2 * i + 2, :] = x_raw[i // 4, i % 4].astype(F32)
    x_ref[...] = x_wide[...].astype(BF16)
    pl.semaphore_wait(barrier, NEAR - 1 + 5)

    send_near(
        near,
        lambda peer: x_ref.at[:, pl.ds(pl.multiple_of(peer * 128, 128), 128)],
        lambda peer: recv_a.at[peer],
        sems, 0,
    )
    recv_a[near] = x_ref[:, pl.ds(pl.multiple_of(near * 128, 128), 128)]

    for step, distance in enumerate((1, 2, 4)):
        greet(ring_sems.at[step], beside(distance, 0))
        greet(ring_sems.at[step], beside(-distance, 0))
        pl.semaphore_wait(ring_sems.at[step], 2)
    greet(ring_sems.at[3], beside(-1, 0))
    pl.semaphore_wait(ring_sems.at[3], 1)
    landed(recv_a.at[pl.ds(0, NEAR - 1)], sems.at[1])

    for pair in range(3):
        rows = []
        for a in (2 * pair, 2 * pair + 1):
            for m in range(NEAR):
                rows.append(recv_a[m].astype(F32)[8 * a : 8 * a + 8])
        turned = jnp.concatenate(rows, axis=0).T
        for fi in range(2):
            stage_b[pl.ds(3 * fi + pair, FAR, stride=8), :] = turned[64 * fi : 64 * fi + 64]
    send_b[...] = stage_b[...].reshape(FAR, 8, 128).astype(BF16)
    send_far(far, lambda peer: send_b.at[peer], lambda peer: recv_c.at[peer], sems, 2, True)
    recv_c[far] = send_b[far]
    for load in loads:
        load.wait()
    for a in range(STA_DEV):
        obs_rows[6 * a : 6 * a + 6, :] = obs_v[a]
    for j in range(4):
        pair = jnp.minimum(4 * seg + j, 35)
        obs_rows[36 + j : 37 + j, :] = obs_rest[pair // 6, pl.ds(pair % 6, 1), :]
    landed(recv_a.at[pl.ds(0, NEAR - 1)], sems.at[0])
    landed(recv_c.at[pl.ds(0, FAR - 1)], sems.at[3])
    stage_b[...] = recv_c[...].astype(F32).reshape(FAR * 8, 128)

    lane32 = lane_iota((32, 128))
    for fi in range(2):
        stations = []
        for pair in range(3):
            both = stage_b[pl.ds(3 * fi + pair, FAR, stride=8), :]
            low, high = both[0:32], both[32:64]
            stations.append(jnp.where(lane32 < 64, low, pltpu.roll(high, 64, 1)))
            stations.append(jnp.where(lane32 < 64, pltpu.roll(low, 64, 1), high))
        stations += [jnp.zeros((32, 128), F32)] * 2
        plain = jnp.concatenate(stations, axis=0)
        even = lax.rem(lane_iota((256, 128)), 2) == 0
        turned = jnp.where(even, pltpu.roll(plain, 127, 1), -pltpu.roll(plain, 1, 1))
        right = plain.astype(BF16)
        for c, left in enumerate((right, turned.astype(BF16))):
            gram = lax.dot_general(right, left, NT, preferred_element_type=F32)
            at = 256 * (2 * fi + c)
            stage_g[0, at : at + 256, :] = gram[:, 0:128]
            stage_g[1, at : at + 256, :] = gram[:, 128:256]

    for a in range(STA_DEV):
        for tile in range(8):
            kept = None
            for i in range(4):
                piece = stage_g[a // 4, pl.ds(4 * tile + i, 32, stride=32), :]
                shift = 32 * ((i - a) % 4)
                piece = pltpu.roll(piece, shift, 1) if shift else piece
                kept = piece if kept is None else jnp.where(lane32 >= 32 * i, piece, kept)
            gram_m[32 * a : 32 * a + 32, 128 * tile : 128 * tile + 128] = kept.astype(BF16)
    gram_m[192:256, :] = jnp.zeros((64, 1024), BF16)

    first = stage_b[pl.ds(6, FAR, stride=8), :]
    second = stage_b[pl.ds(7, FAR, stride=8), :]
    key = (second * 32.0 + first).astype(jnp.int32)
    row64 = lax.broadcasted_iota(jnp.int32, (FAR, 128), 0)
    main_key = jnp.where(row64 < 32, key, pltpu.roll(key, 120, 1))
    lane1024 = lane_iota((FAR, 1024))
    for m in range(NEAR + 1):
        column = key[:, 16:17] if m == NEAR else main_key[:, m : m + 1]
        hit = jnp.where(lane1024 == column, 1.0, 0.0)
        onehot[64 * m : 64 * m + 64, :] = hit.astype(BF16)
    slots = lax.dot_general(onehot[...], gram_m[...], NT, preferred_element_type=F32)
    slots = slots.astype(BF16)
    kept = jnp.dot(slots[0:512], maps_v[0], preferred_element_type=F32)
    for m in range(NEAR):
        stage_f[pl.ds(m, FAR, stride=16), :] = kept[64 * m : 64 * m + 64]
    rest = slots[512:576]
    upper = lax.broadcasted_iota(jnp.int32, (FAR, 256), 0) < 32
    rest_low = jnp.where(upper, rest, jnp.zeros_like(rest))
    rest_high = jnp.where(upper, jnp.zeros_like(rest), rest)
    for h in range(2):
        tail = jnp.dot(rest_low, maps_v[5 + h], preferred_element_type=F32)
        if h == 0:
            tail = tail + jnp.dot(rest_high, maps_v[7], preferred_element_type=F32)
        for i in range(4):
            at = 64 * (4 * h + i)
            tail = tail + jnp.dot(
                slots[at : at + 64], maps_v[1 + i], preferred_element_type=F32
            )
        stage_f[pl.ds(8 + h, FAR, stride=16), :] = tail
    send_f[...] = stage_f[...].astype(BF16)

    def chunk16(ref):
        return lambda peer: ref.at[pl.ds(pl.multiple_of(peer * 16, 16), 10), :]

    send_far(far, chunk16(send_f), chunk16(recv_f), sems, 4, True)
    own = pl.ds(pl.multiple_of(far * 16, 16), 16)
    recv_f[own, :] = send_f[own, :]
    landed(send_b.at[pl.ds(0, FAR - 1)], sems.at[2])
    landed(recv_f.at[pl.ds(0, 10 * (FAR - 1))], sems.at[5])
    stage_f[...] = recv_f[...].astype(F32)
    lane16 = lane_iota((16, 128))
    tails = [stage_f[pl.ds(8 + h, FAR, stride=16), :] for h in range(2)]
    for m in range(NEAR):
        send_g[m, 0:64, :] = stage_f[pl.ds(m, FAR, stride=16), :].astype(BF16)
        packed = None
        for i in range(4):
            piece = tails[m // 4][16 * i : 16 * i + 16]
            shift = 32 * ((i - m) % 4)
            piece = pltpu.roll(piece, shift, 1) if shift else piece
            packed = piece if packed is None else jnp.where(lane16 >= 32 * i, piece, packed)
        send_g[m, 64:80, :] = packed.astype(BF16)
    send_near(near, lambda peer: send_g.at[peer], lambda peer: recv_g.at[peer], sems, 6)
    recv_g[near] = send_g[near]
    landed(send_f.at[pl.ds(0, 10 * (FAR - 1))], sems.at[4])
    landed(recv_g.at[pl.ds(0, NEAR - 1)], sems.at[7])

    tail_rows = []
    for m in range(NEAR):
        blocks = recv_g[m, 64:80, :].astype(F32)
        for i in range(4):
            shift = 32 * ((m - i) % 4)
            tail_rows.append(pltpu.roll(blocks, shift, 1) if shift else blocks)
    lane128 = lane_iota((128, 128))
    tail = None
    for xt in range(4):
        both = jnp.concatenate(tail_rows[4 * xt : 4 * xt + 4] + tail_rows[4 * xt + 16 : 4 * xt + 20])
        tail = both if tail is None else jnp.where(lane128 >= 32 * xt, both, tail)
    tail = tail.T
    for xt in range(4):
        lanes = slice(128 * xt, 128 * xt + 128)
        square = jnp.concatenate(
            [recv_g[xt, 0:64, :].astype(F32), recv_g[4 + xt, 0:64, :].astype(F32)], axis=0
        ).T
        for fc in range(4):
            s_ref[fc, 0:32, lanes] = square[32 * fc : 32 * fc + 32]
            s_ref[fc, 32:40, lanes] = tail[32 * xt + 8 * fc : 32 * xt + 8 * fc + 8]
    lags = jnp.zeros((40, LAGS), F32)
    for fc in range(4):
        lags = lags + jnp.dot(s_ref[fc].astype(BF16), kern_v[fc], preferred_element_type=F32)

    def floor_of(slot):
        p, q = pairs_ref[0, slot], pairs_ref[1, slot]
        return jnp.where(p < 0, 99, jnp.where(p != q, -99, 0))

    row = lax.broadcasted_iota(jnp.int32, (40, LAGS), 0)
    pair = jnp.where(row < 36, row, jnp.minimum(row - 36 + 4 * seg, 35))
    floor = jnp.where(row < 36, floor_of(seg), jnp.where(seg < 9, floor_of(16), 99))
    keep = pair - 7 * sixths(pair) > floor
    value = jnp.tanh(SCALE * lags - obs_rows[...])
    residual = jnp.where(keep, value, 0.0).astype(BF16)

    to = lax.broadcasted_iota(jnp.int32, (16, 40), 0)
    of = lane_iota((16, 40))
    first_of = sixths(of)
    main = of < 36
    picked = (to < 6) & main & (first_of == to)
    picked = picked | ((to >= 6) & (to < 12) & main & (of - 6 * first_of == to - 6))
    picked = picked | ((of >= 36) & (of - 36 == to - 12))
    picked = jnp.where(picked, 1.0, 0.0).astype(BF16)
    for fi in range(2):
        gamma = [
            SCALE * lax.dot_general(residual, kern_v[2 * fi + c], NT, preferred_element_type=F32)
            for c in range(2)
        ]
        s0, s1 = s_ref[2 * fi], s_ref[2 * fi + 1]
        common = gamma[0] * s0 + gamma[1] * s1
        twist = gamma[1] * s0 - gamma[0] * s1
        for ct, term in enumerate((common, twist)):
            block = sum(
                jnp.dot(picked, third, preferred_element_type=F32) for third in thirds(term)
            )
            for xt in range(4):
                send_i[2 * xt + fi, 16 * ct : 16 * ct + 16, :] = block[:, 128 * xt : 128 * xt + 128]
    send_near(near, lambda peer: send_i.at[peer], lambda peer: recv_i.at[peer], sems, 8)
    recv_i[near] = send_i[near]

    lane = lane_iota((1, 128))
    source = lax.shift_right_logical(lane, 4)
    t = lane - 16 * source
    p_main = jnp.full((1, 128), -1, jnp.int32)
    q_main = p_main
    for m in range(NEAR):
        p_main = jnp.where(source == m, pairs_ref[0, zh * 8 + m], p_main)
        q_main = jnp.where(source == m, pairs_ref[1, zh * 8 + m], q_main)
    pair = jnp.clip(32 * zh + 4 * source + t - 12, 0, 35)
    valid = 32 * zh + 4 * source + t - 12 < 36
    a_rest = sixths(pair)
    plus = jnp.where(
        t < 6, 8 * p_main + t,
        jnp.where((t >= 12) & valid, 8 * pairs_ref[0, 16] + a_rest, -1),
    )
    minus = jnp.where(
        (t >= 6) & (t < 12), 8 * q_main + t - 6,
        jnp.where((t >= 12) & valid, 8 * pairs_ref[1, 16] + pair - 6 * a_rest, -1),
    )
    station = lax.broadcasted_iota(jnp.int32, (256, 128), 0)
    plus = jnp.where(station == plus, 1.0, 0.0)
    minus = jnp.where(station == minus, 1.0, 0.0)
    choose = ((plus + minus).astype(BF16), (plus - minus).astype(BF16))
    landed(send_g.at[pl.ds(0, NEAR - 1)], sems.at[6])
    landed(recv_i.at[pl.ds(0, NEAR - 1)], sems.at[9])
    sums = []
    for ct in range(2):
        terms = recv_i[:, 16 * ct : 16 * ct + 16, :].reshape(128, 128)
        sums.append(
            sum(jnp.dot(choose[ct], third, preferred_element_type=F32) for third in thirds(terms))
        )
    lane256 = lane_iota((256, 128))
    send_k[0:256, :] = jnp.where(lane256 < 64, sums[0], pltpu.roll(sums[1], 64, 1))
    send_k[256:512, :] = jnp.where(lane256 < 64, pltpu.roll(sums[0], 64, 1), sums[1])

    def chunk8(ref):
        return lambda peer: ref.at[pl.ds(pl.multiple_of(peer * 8, 8), STA_DEV), :]

    send_far(far, chunk8(send_k), chunk8(recv_k), sems, 10, True)
    own = pl.ds(pl.multiple_of(far * 8, 8), 8)
    recv_k[own, :] = send_k[own, :]
    landed(send_i.at[pl.ds(0, NEAR - 1)], sems.at[8])
    landed(recv_k.at[pl.ds(0, STA_DEV * (FAR - 1))], sems.at[11])
    total = recv_k[0:8, :]
    for k in range(1, FAR):
        total = total + recv_k[8 * k : 8 * k + 8, :]
    out_ref[:, 0, :] = total[0:STA_DEV, 0:64]
    out_ref[:, 1, :] = total[0:STA_DEV, 64:128]
    landed(send_k.at[pl.ds(0, STA_DEV * (FAR - 1))], sems.at[10])


def on_device(spectra, observed, pair_table):
    vmem = pl.BlockSpec(memory_space=pltpu.VMEM)
    hbm = pl.BlockSpec(memory_space=pl.ANY)
    return pl.pallas_call(
        body,
        out_shape=pltpu.VMEM((STA_DEV, 2, 64), F32),
        in_specs=[hbm] * 5,
        out_specs=vmem,
        scratch_shapes=[
            pltpu.VMEM((6, 4, 2, 1024), BF16),
            pltpu.VMEM((48, 1024), F32),
            pltpu.VMEM((48, 1024), BF16),
            pltpu.VMEM((8, 48, 128), BF16),
            pltpu.VMEM((64, 8, 128), BF16),
            pltpu.VMEM((64, 8, 128), BF16),
            pltpu.VMEM((512, 128), F32),
            pltpu.VMEM((2, 1024, 128), F32),
            pltpu.VMEM((256, 1024), BF16),
            pltpu.VMEM((576, 1024), BF16),
            pltpu.VMEM((1024, 128), F32),
            pltpu.VMEM((1024, 128), BF16),
            pltpu.VMEM((1024, 128), BF16),
            pltpu.VMEM((8, 80, 128), BF16),
            pltpu.VMEM((8, 80, 128), BF16),
            pltpu.VMEM((4, 40, 512), F32),
            pltpu.VMEM((8, 32, 128), F32),
            pltpu.VMEM((8, 32, 128), F32),
            pltpu.VMEM((512, 128), F32),
            pltpu.VMEM((512, 128), F32),
            pltpu.VMEM((6, 6, 512), F32),
            pltpu.VMEM((6, 6, 512), F32),
            pltpu.VMEM((40, 512), F32),
            pltpu.VMEM((4, 512, 512), BF16),
            pltpu.VMEM((8, 256, 128), BF16),
            pltpu.SMEM((2, 17), jnp.int32),
            pltpu.SemaphoreType.DMA((6,)),
            pltpu.SemaphoreType.DMA((12,)),
            pltpu.SemaphoreType.REGULAR((4,)),
        ],
        compiler_params=pltpu.CompilerParams(collective_id=0, has_side_effects=True),
    )(spectra, pair_table.T, observed, lag_kernel(), lane_maps())


def solution(mesh):
    torus = Mesh(mesh.devices.reshape(8, 4, 2, 4, 2), ("sta_0", "sta_1", "seg_0", "seg_1", "seg_2"))
    in_specs = (P(STA, SEG, None, None), P(STA, None, None, None), P(STA, None))
    out_specs = P(STA, None, SEG)
    return jax.shard_map(
        on_device, mesh=torus, in_specs=in_specs, out_specs=out_specs, check_vma=False
    )
```

```python
import math

import jax
import jax.numpy as jnp
import numpy as np
from jax import lax
from jax.experimental import pallas as pl
from jax.experimental.pallas import tpu as pltpu
from jax.sharding import Mesh
from jax.sharding import PartitionSpec as P

F = 1024
LAGS = 512
STA_DEV = 6
SEGS = 64
SEG = ("seg_0", "seg_1", "seg_2")
STA = ("sta_0", "sta_1")
SCALE = 1.0 / math.sqrt(F * SEGS)
NEAR = 8
FAR = 64
PITCH = 40
F32 = jnp.float32
BF16 = jnp.bfloat16
NT = (((1,), (1,)), ((), ()))


def lag_kernel():
    frequency = np.arange(F, dtype=np.int32)[:, None]
    offset = np.arange(LAGS, dtype=np.int32)[None, :] - LAGS // 2
    phase = np.mod(frequency * offset, 2 * F)
    angle = np.float32(math.pi / F) * phase.astype(np.float32)
    kernel = np.stack([np.cos(angle), -np.sin(angle)], axis=0)
    kernel = kernel.reshape(2, 2, 4, 2, 64, LAGS).transpose(3, 0, 2, 1, 4, 5)
    return jnp.asarray(kernel.reshape(4, 512, LAGS).astype(BF16))


def lane_maps():
    maps = np.zeros((8, 256, 128), np.float32)
    for a in range(STA_DEV):
        for b in range(STA_DEV):
            pair = STA_DEV * a + b
            for fc in range(4):
                row = 32 * a + 8 * fc + b
                if pair < 32:
                    maps[0, row, 32 * fc + pair] = 1
                    h, i, j = pair // 16, pair // 4 % 4, pair % 4
                    maps[5 + h, row, 32 * i + 8 * fc + 4 + j] = 1
                else:
                    for i in range(4):
                        maps[1 + i, row, 32 * i + 8 * fc + pair - 32] = 1
                    maps[7, row, 8 * fc + 4 + pair - 32] = 1
    return jnp.asarray(maps.astype(BF16))


def thirds(value):
    first = value.astype(BF16)
    rest = value - first.astype(F32)
    second = rest.astype(BF16)
    return first, second, (rest - second.astype(F32)).astype(BF16)


def sixths(index):
    return sum((index >= 6 * i).astype(jnp.int32) for i in range(1, 6))


def far_id(index):
    return {"seg_0": index // 32, "sta_0": (index // 4) % 8, "sta_1": index % 4}


def near_id(index):
    return {"seg_1": index // 2, "seg_2": index % 2}


def landed(ref, semaphore):
    pltpu.make_async_copy(ref, ref, semaphore).wait()


def send(source, target, semaphores, at, device):
    pltpu.make_async_remote_copy(
        src_ref=source,
        dst_ref=target,
        send_sem=semaphores.at[at],
        recv_sem=semaphores.at[at + 1],
        device_id=device,
        device_id_type=pl.DeviceIdType.MESH,
    ).start()


def send_near(me, source, target, semaphores, at):
    x, core = me // 2, lax.rem(me, 2)
    for dx, change in ((2, 1), (2, 0), (1, 1), (3, 1), (1, 0), (3, 0), (0, 1)):
        peer = lax.rem(x + dx, 4) * 2 + (1 - core if change else core)
        send(source(peer), target(me), semaphores, at, near_id(peer))


def send_far(me, source, target, semaphores, at, farthest_first):
    z, y = me // 4, lax.rem(me, 4)
    ys = [lax.rem(y + dy, 4) for dy in range(4)]

    def to_chip(peer_z, dys):
        zh, zl = peer_z // 8, lax.rem(peer_z, 8)
        for dy in dys:
            peer = peer_z * 4 + ys[dy]
            device = {"seg_0": zh, "sta_0": zl, "sta_1": ys[dy]}
            send(source(peer), target(me), semaphores, at, device)

    def step(j, carry):
        if farthest_first:
            j = 16 - j
            dz = (j + 1) // 2 * (1 - 2 * lax.rem(j + 1, 2))
            to_chip(lax.rem(z + dz + 16, 16), (2, 1, 3, 0))
        else:
            to_chip(lax.rem(z + j, 16), range(4))
        return carry

    lax.fori_loop(1, 16, step, 0)
    to_chip(z, (2, 1, 3))


def lane_iota(shape):
    return lax.broadcasted_iota(jnp.int32, shape, len(shape) - 1)


def body(
    x_hbm, pairs_hbm, observed_ref, kernel_ref, maps_ref, out_ref,
    x_raw, x_wide, x_ref, recv_a, send_b, recv_c, stage_b, stage_g, gram_m, onehot,
    stage_f, send_f, recv_f, send_g, recv_g, s_ref, send_i, recv_i, send_k, recv_k,
    obs_v, obs_rest, obs_rows, kern_v, maps_v, pairs_ref,
    local_sems, sems, ring_sems,
):
    zh = lax.axis_index("seg_0")
    far = zh * 32 + lax.axis_index("sta_0") * 4 + lax.axis_index("sta_1")
    near = lax.axis_index("seg_1") * 2 + lax.axis_index("seg_2")
    seg = zh * 8 + near

    load_x = pltpu.make_async_copy(x_hbm, x_raw, local_sems.at[0])
    load_pairs = pltpu.make_async_copy(pairs_hbm, pairs_ref, local_sems.at[1])
    loads = [
        pltpu.make_async_copy(observed_ref.at[seg], obs_v, local_sems.at[2]),
        pltpu.make_async_copy(observed_ref.at[16], obs_rest, local_sems.at[3]),
        pltpu.make_async_copy(kernel_ref, kern_v, local_sems.at[4]),
        pltpu.make_async_copy(maps_ref, maps_v, local_sems.at[5]),
    ]
    barrier = pltpu.get_barrier_semaphore()

    z, y = far // 4, far % 4

    def beside(dz, dy):
        return far_id(lax.rem(z + dz + 16, 16) * 4 + lax.rem(y + dy, 4))

    def greet(semaphore, device):
        pl.semaphore_signal(
            semaphore, inc=1, device_id=device, device_id_type=pl.DeviceIdType.MESH
        )

    for i in range(1, NEAR):
        greet(barrier, near_id(lax.rem(near + i, NEAR)))
    for dy in (1, 2, 3):
        greet(barrier, beside(0, dy))
    for dz in (1, -1):
        greet(barrier, beside(dz, 0))
    load_x.start()
    load_pairs.start()
    for load in loads:
        load.start()
    load_pairs.wait()
    lane = lane_iota((1, 128))
    for end in range(2):
        row = jnp.zeros((1, 128), F32)
        for slot in range(17):
            row = jnp.where(lane == slot, pairs_ref[end, slot].astype(F32), row)
        stage_b[pl.ds(6 + end, FAR, stride=8), :] = jnp.broadcast_to(row, (FAR, 128))
    load_x.wait()
    for i in range(24):
        x_wide[2 * i : 2 * i + 2, :] = x_raw[i // 4, i % 4].astype(F32)
    x_ref[...] = x_wide[...].astype(BF16)
    pl.semaphore_wait(barrier, NEAR - 1 + 5)

    send_near(
        near,
        lambda peer: x_ref.at[:, pl.ds(pl.multiple_of(peer * 128, 128), 128)],
        lambda peer: recv_a.at[peer],
        sems, 0,
    )
    recv_a[near] = x_ref[:, pl.ds(pl.multiple_of(near * 128, 128), 128)]

    for step, distance in enumerate((1, 2, 4)):
        greet(ring_sems.at[step], beside(distance, 0))
        greet(ring_sems.at[step], beside(-distance, 0))
        pl.semaphore_wait(ring_sems.at[step], 2)
    greet(ring_sems.at[3], beside(-1, 0))
    pl.semaphore_wait(ring_sems.at[3], 1)
    landed(recv_a.at[pl.ds(0, NEAR - 1)], sems.at[1])

    for pair in range(3):
        rows = []
        for a in (2 * pair, 2 * pair + 1):
            for m in range(NEAR):
                rows.append(recv_a[m].astype(F32)[8 * a : 8 * a + 8])
        turned = jnp.concatenate(rows, axis=0).T
        for fi in range(2):
            stage_b[pl.ds(3 * fi + pair, FAR, stride=8), :] = turned[64 * fi : 64 * fi + 64]
    send_b[...] = stage_b[...].reshape(FAR, 8, 128).astype(BF16)
    send_far(far, lambda peer: send_b.at[peer], lambda peer: recv_c.at[peer], sems, 2, True)
    recv_c[far] = send_b[far]
    for load in loads:
        load.wait()
    for a in range(STA_DEV):
        obs_rows[6 * a : 6 * a + 6, :] = obs_v[a]
    for j in range(4):
        pair = jnp.minimum(4 * seg + j, 35)
        obs_rows[36 + j : 37 + j, :] = obs_rest[pair // 6, pl.ds(pair % 6, 1), :]
    landed(recv_a.at[pl.ds(0, NEAR - 1)], sems.at[0])
    landed(recv_c.at[pl.ds(0, FAR - 1)], sems.at[3])
    stage_b[...] = recv_c[...].astype(F32).reshape(FAR * 8, 128)

    lane32 = lane_iota((32, 128))
    for fi in range(2):
        stations = []
        for pair in range(3):
            both = stage_b[pl.ds(3 * fi + pair, FAR, stride=8), :]
            low, high = both[0:32], both[32:64]
            stations.append(jnp.where(lane32 < 64, low, pltpu.roll(high, 64, 1)))
            stations.append(jnp.where(lane32 < 64, pltpu.roll(low, 64, 1), high))
        stations += [jnp.zeros((32, 128), F32)] * 2
        plain = jnp.concatenate(stations, axis=0)
        even = lax.rem(lane_iota((256, 128)), 2) == 0
        turned = jnp.where(even, pltpu.roll(plain, 127, 1), -pltpu.roll(plain, 1, 1))
        right = plain.astype(BF16)
        for c, left in enumerate((right, turned.astype(BF16))):
            gram = lax.dot_general(right, left, NT, preferred_element_type=F32)
            for i in range(8):
                at = PITCH * (8 * (2 * fi + c) + i)
                stage_g[0, at : at + 32, :] = gram[32 * i : 32 * i + 32, 0:128]
                stage_g[1, at : at + 32, :] = gram[32 * i : 32 * i + 32, 128:256]

    for tile in range(8):
        for half in range(2):
            pieces = [
                stage_g[half, pl.ds(4 * tile + i, 32, stride=PITCH), :] for i in range(4)
            ]
            for a in range(4 * half, min(4 * half + 4, STA_DEV)):
                kept = None
                for i, piece in enumerate(pieces):
                    shift = 32 * ((i - a) % 4)
                    piece = pltpu.roll(piece, shift, 1) if shift else piece
                    kept = piece if kept is None else jnp.where(lane32 >= 32 * i, piece, kept)
                gram_m[32 * a : 32 * a + 32, 128 * tile : 128 * tile + 128] = kept.astype(BF16)
    gram_m[192:256, :] = jnp.zeros((64, 1024), BF16)

    first = stage_b[pl.ds(6, FAR, stride=8), :]
    second = stage_b[pl.ds(7, FAR, stride=8), :]
    key = (second * 32.0 + first).astype(jnp.int32)
    row64 = lax.broadcasted_iota(jnp.int32, (FAR, 128), 0)
    main_key = jnp.where(row64 < 32, key, pltpu.roll(key, 120, 1))
    lane1024 = lane_iota((FAR, 1024))
    for m in range(NEAR + 1):
        column = key[:, 16:17] if m == NEAR else main_key[:, m : m + 1]
        hit = jnp.where(lane1024 == column, 1.0, 0.0)
        onehot[64 * m : 64 * m + 64, :] = hit.astype(BF16)
    slots = lax.dot_general(onehot[...], gram_m[...], NT, preferred_element_type=F32)
    slots = slots.astype(BF16)
    kept = jnp.dot(slots[0:512], maps_v[0], preferred_element_type=F32)
    for m in range(NEAR):
        stage_f[pl.ds(m, FAR, stride=16), :] = kept[64 * m : 64 * m + 64]
    rest = slots[512:576]
    upper = lax.broadcasted_iota(jnp.int32, (FAR, 256), 0) < 32
    rest_low = jnp.where(upper, rest, jnp.zeros_like(rest))
    rest_high = jnp.where(upper, jnp.zeros_like(rest), rest)
    for h in range(2):
        tail = jnp.dot(rest_low, maps_v[5 + h], preferred_element_type=F32)
        if h == 0:
            tail = tail + jnp.dot(rest_high, maps_v[7], preferred_element_type=F32)
        for i in range(4):
            at = 64 * (4 * h + i)
            tail = tail + jnp.dot(
                slots[at : at + 64], maps_v[1 + i], preferred_element_type=F32
            )
        stage_f[pl.ds(8 + h, FAR, stride=16), :] = tail
    send_f[...] = stage_f[...].astype(BF16)

    def chunk16(ref):
        return lambda peer: ref.at[pl.ds(pl.multiple_of(peer * 16, 16), 10), :]

    send_far(far, chunk16(send_f), chunk16(recv_f), sems, 4, True)
    own = pl.ds(pl.multiple_of(far * 16, 16), 16)
    recv_f[own, :] = send_f[own, :]
    landed(send_b.at[pl.ds(0, FAR - 1)], sems.at[2])
    landed(recv_f.at[pl.ds(0, 10 * (FAR - 1))], sems.at[5])
    stage_f[...] = recv_f[...].astype(F32)
    lane16 = lane_iota((16, 128))
    tails = [stage_f[pl.ds(8 + h, FAR, stride=16), :] for h in range(2)]
    for m in range(NEAR):
        send_g[m, 0:64, :] = stage_f[pl.ds(m, FAR, stride=16), :].astype(BF16)
        packed = None
        for i in range(4):
            piece = tails[m // 4][16 * i : 16 * i + 16]
            shift = 32 * ((i - m) % 4)
            piece = pltpu.roll(piece, shift, 1) if shift else piece
            packed = piece if packed is None else jnp.where(lane16 >= 32 * i, piece, packed)
        send_g[m, 64:80, :] = packed.astype(BF16)
    send_near(near, lambda peer: send_g.at[peer], lambda peer: recv_g.at[peer], sems, 6)
    recv_g[near] = send_g[near]
    landed(send_f.at[pl.ds(0, 10 * (FAR - 1))], sems.at[4])
    landed(recv_g.at[pl.ds(0, NEAR - 1)], sems.at[7])

    tail_rows = []
    for m in range(NEAR):
        blocks = recv_g[m, 64:80, :].astype(F32)
        for i in range(4):
            shift = 32 * ((m - i) % 4)
            tail_rows.append(pltpu.roll(blocks, shift, 1) if shift else blocks)
    lane128 = lane_iota((128, 128))
    tail = None
    for xt in range(4):
        both = jnp.concatenate(tail_rows[4 * xt : 4 * xt + 4] + tail_rows[4 * xt + 16 : 4 * xt + 20])
        tail = both if tail is None else jnp.where(lane128 >= 32 * xt, both, tail)
    tail = tail.T
    for xt in range(4):
        lanes = slice(128 * xt, 128 * xt + 128)
        square = jnp.concatenate(
            [recv_g[xt, 0:64, :].astype(F32), recv_g[4 + xt, 0:64, :].astype(F32)], axis=0
        ).T
        for fc in range(4):
            s_ref[fc, 0:32, lanes] = square[32 * fc : 32 * fc + 32]
            s_ref[fc, 32:40, lanes] = tail[32 * xt + 8 * fc : 32 * xt + 8 * fc + 8]
    lags = jnp.zeros((40, LAGS), F32)
    for fc in range(4):
        lags = lags + jnp.dot(s_ref[fc].astype(BF16), kern_v[fc], preferred_element_type=F32)

    def floor_of(slot):
        p, q = pairs_ref[0, slot], pairs_ref[1, slot]
        return jnp.where(p < 0, 99, jnp.where(p != q, -99, 0))

    row = lax.broadcasted_iota(jnp.int32, (40, LAGS), 0)
    pair = jnp.where(row < 36, row, jnp.minimum(row - 36 + 4 * seg, 35))
    floor = jnp.where(row < 36, floor_of(seg), jnp.where(seg < 9, floor_of(16), 99))
    keep = pair - 7 * sixths(pair) > floor
    value = jnp.tanh(SCALE * lags - obs_rows[...])
    residual = jnp.where(keep, value, 0.0).astype(BF16)

    to = lax.broadcasted_iota(jnp.int32, (16, 40), 0)
    of = lane_iota((16, 40))
    first_of = sixths(of)
    main = of < 36
    picked = (to < 6) & main & (first_of == to)
    picked = picked | ((to >= 6) & (to < 12) & main & (of - 6 * first_of == to - 6))
    picked = picked | ((of >= 36) & (of - 36 == to - 12))
    picked = jnp.where(picked, 1.0, 0.0).astype(BF16)
    for fi in range(2):
        gamma = [
            SCALE * lax.dot_general(residual, kern_v[2 * fi + c], NT, preferred_element_type=F32)
            for c in range(2)
        ]
        s0, s1 = s_ref[2 * fi], s_ref[2 * fi + 1]
        common = gamma[0] * s0 + gamma[1] * s1
        twist = gamma[1] * s0 - gamma[0] * s1
        for ct, term in enumerate((common, twist)):
            block = sum(
                jnp.dot(picked, third, preferred_element_type=F32) for third in thirds(term)
            )
            for xt in range(4):
                send_i[2 * xt + fi, 16 * ct : 16 * ct + 16, :] = block[:, 128 * xt : 128 * xt + 128]
    send_near(near, lambda peer: send_i.at[peer], lambda peer: recv_i.at[peer], sems, 8)
    recv_i[near] = send_i[near]

    lane = lane_iota((1, 128))
    source = lax.shift_right_logical(lane, 4)
    t = lane - 16 * source
    p_main = jnp.full((1, 128), -1, jnp.int32)
    q_main = p_main
    for m in range(NEAR):
        p_main = jnp.where(source == m, pairs_ref[0, zh * 8 + m], p_main)
        q_main = jnp.where(source == m, pairs_ref[1, zh * 8 + m], q_main)
    pair = jnp.clip(32 * zh + 4 * source + t - 12, 0, 35)
    valid = 32 * zh + 4 * source + t - 12 < 36
    a_rest = sixths(pair)
    plus = jnp.where(
        t < 6, 8 * p_main + t,
        jnp.where((t >= 12) & valid, 8 * pairs_ref[0, 16] + a_rest, -1),
    )
    minus = jnp.where(
        (t >= 6) & (t < 12), 8 * q_main + t - 6,
        jnp.where((t >= 12) & valid, 8 * pairs_ref[1, 16] + pair - 6 * a_rest, -1),
    )
    station = lax.broadcasted_iota(jnp.int32, (256, 128), 0)
    plus = jnp.where(station == plus, 1.0, 0.0)
    minus = jnp.where(station == minus, 1.0, 0.0)
    choose = ((plus + minus).astype(BF16), (plus - minus).astype(BF16))
    landed(send_g.at[pl.ds(0, NEAR - 1)], sems.at[6])
    landed(recv_i.at[pl.ds(0, NEAR - 1)], sems.at[9])
    sums = []
    for ct in range(2):
        terms = recv_i[:, 16 * ct : 16 * ct + 16, :].reshape(128, 128)
        sums.append(
            sum(jnp.dot(choose[ct], third, preferred_element_type=F32) for third in thirds(terms))
        )
    lane256 = lane_iota((256, 128))
    send_k[0:256, :] = jnp.where(lane256 < 64, sums[0], pltpu.roll(sums[1], 64, 1))
    send_k[256:512, :] = jnp.where(lane256 < 64, pltpu.roll(sums[0], 64, 1), sums[1])

    def chunk8(ref):
        return lambda peer: ref.at[pl.ds(pl.multiple_of(peer * 8, 8), STA_DEV), :]

    send_far(far, chunk8(send_k), chunk8(recv_k), sems, 10, True)
    own = pl.ds(pl.multiple_of(far * 8, 8), 8)
    recv_k[own, :] = send_k[own, :]
    landed(send_i.at[pl.ds(0, NEAR - 1)], sems.at[8])
    landed(recv_k.at[pl.ds(0, STA_DEV * (FAR - 1))], sems.at[11])
    total = recv_k[0:8, :]
    for k in range(1, FAR):
        total = total + recv_k[8 * k : 8 * k + 8, :]
    out_ref[:, 0, :] = total[0:STA_DEV, 0:64]
    out_ref[:, 1, :] = total[0:STA_DEV, 64:128]
    landed(send_k.at[pl.ds(0, STA_DEV * (FAR - 1))], sems.at[10])


def on_device(spectra, observed, pair_table):
    vmem = pl.BlockSpec(memory_space=pltpu.VMEM)
    hbm = pl.BlockSpec(memory_space=pl.ANY)
    return pl.pallas_call(
        body,
        out_shape=pltpu.VMEM((STA_DEV, 2, 64), F32),
        in_specs=[hbm] * 5,
        out_specs=vmem,
        scratch_shapes=[
            pltpu.VMEM((6, 4, 2, 1024), BF16),
            pltpu.VMEM((48, 1024), F32),
            pltpu.VMEM((48, 1024), BF16),
            pltpu.VMEM((8, 48, 128), BF16),
            pltpu.VMEM((64, 8, 128), BF16),
            pltpu.VMEM((64, 8, 128), BF16),
            pltpu.VMEM((512, 128), F32),
            pltpu.VMEM((2, 32 * PITCH, 128), F32),
            pltpu.VMEM((256, 1024), BF16),
            pltpu.VMEM((576, 1024), BF16),
            pltpu.VMEM((1024, 128), F32),
            pltpu.VMEM((1024, 128), BF16),
            pltpu.VMEM((1024, 128), BF16),
            pltpu.VMEM((8, 80, 128), BF16),
            pltpu.VMEM((8, 80, 128), BF16),
            pltpu.VMEM((4, 40, 512), F32),
            pltpu.VMEM((8, 32, 128), F32),
            pltpu.VMEM((8, 32, 128), F32),
            pltpu.VMEM((512, 128), F32),
            pltpu.VMEM((512, 128), F32),
            pltpu.VMEM((6, 6, 512), F32),
            pltpu.VMEM((6, 6, 512), F32),
            pltpu.VMEM((40, 512), F32),
            pltpu.VMEM((4, 512, 512), BF16),
            pltpu.VMEM((8, 256, 128), BF16),
            pltpu.SMEM((2, 17), jnp.int32),
            pltpu.SemaphoreType.DMA((6,)),
            pltpu.SemaphoreType.DMA((12,)),
            pltpu.SemaphoreType.REGULAR((4,)),
        ],
        compiler_params=pltpu.CompilerParams(collective_id=0, has_side_effects=True),
    )(spectra, pair_table.T, observed, lag_kernel(), lane_maps())


def solution(mesh):
    torus = Mesh(mesh.devices.reshape(8, 4, 2, 4, 2), ("sta_0", "sta_1", "seg_0", "seg_1", "seg_2"))
    in_specs = (P(STA, SEG, None, None), P(STA, None, None, None), P(STA, None))
    out_specs = P(STA, None, SEG)
    return jax.shard_map(
        on_device, mesh=torus, in_specs=in_specs, out_specs=out_specs, check_vma=False
    )
```

```python
import math

import jax
import jax.numpy as jnp
import numpy as np
from jax import lax
from jax.experimental import pallas as pl
from jax.experimental.pallas import tpu as pltpu
from jax.sharding import Mesh
from jax.sharding import PartitionSpec as P

F = 1024
LAGS = 512
STA_DEV = 6
SEGS = 64
SEG = ("seg_0", "seg_1", "seg_2")
STA = ("sta_0", "sta_1")
SCALE = 1.0 / math.sqrt(F * SEGS)
NEAR = 8
FAR = 64
PITCH = 40
F32 = jnp.float32
BF16 = jnp.bfloat16
NT = (((1,), (1,)), ((), ()))


def lag_kernel():
    frequency = np.arange(F, dtype=np.int32)[:, None]
    offset = np.arange(LAGS, dtype=np.int32)[None, :] - LAGS // 2
    phase = np.mod(frequency * offset, 2 * F)
    angle = np.float32(math.pi / F) * phase.astype(np.float32)
    kernel = np.stack([np.cos(angle), -np.sin(angle)], axis=0)
    kernel = kernel.reshape(2, 2, 4, 2, 64, LAGS).transpose(3, 0, 2, 1, 4, 5)
    return jnp.asarray(kernel.reshape(4, 512, LAGS).astype(BF16))


def lane_maps():
    maps = np.zeros((8, 256, 128), np.float32)
    for a in range(STA_DEV):
        for b in range(STA_DEV):
            pair = STA_DEV * a + b
            for fc in range(4):
                row = 32 * a + 8 * fc + b
                if pair < 32:
                    maps[0, row, 32 * fc + pair] = 1
                    h, i, j = pair // 16, pair // 4 % 4, pair % 4
                    maps[5 + h, row, 32 * i + 8 * fc + 4 + j] = 1
                else:
                    for i in range(4):
                        maps[1 + i, row, 32 * i + 8 * fc + pair - 32] = 1
                    maps[7, row, 8 * fc + 4 + pair - 32] = 1
    return jnp.asarray(maps.astype(BF16))


def thirds(value):
    first = value.astype(BF16)
    rest = value - first.astype(F32)
    second = rest.astype(BF16)
    return first, second, (rest - second.astype(F32)).astype(BF16)


def sixths(index):
    return sum((index >= 6 * i).astype(jnp.int32) for i in range(1, 6))


def far_id(index):
    return {"seg_0": index // 32, "sta_0": (index // 4) % 8, "sta_1": index % 4}


def near_id(index):
    return {"seg_1": index // 2, "seg_2": index % 2}


def landed(ref, semaphore):
    pltpu.make_async_copy(ref, ref, semaphore).wait()


def send(source, target, semaphores, at, device):
    pltpu.make_async_remote_copy(
        src_ref=source,
        dst_ref=target,
        send_sem=semaphores.at[at],
        recv_sem=semaphores.at[at + 1],
        device_id=device,
        device_id_type=pl.DeviceIdType.MESH,
    ).start()


def send_near(me, source, target, semaphores, at):
    x, core = me // 2, lax.rem(me, 2)
    for dx, change in ((2, 1), (2, 0), (1, 1), (3, 1), (1, 0), (3, 0), (0, 1)):
        peer = lax.rem(x + dx, 4) * 2 + (1 - core if change else core)
        send(source(peer), target(me), semaphores, at, near_id(peer))


def send_far(me, source, target, semaphores, at, farthest_first):
    z, y = me // 4, lax.rem(me, 4)
    ys = [lax.rem(y + dy, 4) for dy in range(4)]

    def to_chip(peer_z, dys):
        zh, zl = peer_z // 8, lax.rem(peer_z, 8)
        for dy in dys:
            peer = peer_z * 4 + ys[dy]
            device = {"seg_0": zh, "sta_0": zl, "sta_1": ys[dy]}
            send(source(peer), target(me), semaphores, at, device)

    def step(j, carry):
        if farthest_first:
            j = 16 - j
            dz = (j + 1) // 2 * (1 - 2 * lax.rem(j + 1, 2))
            to_chip(lax.rem(z + dz + 16, 16), (2, 1, 3, 0))
        else:
            to_chip(lax.rem(z + j, 16), range(4))
        return carry

    lax.fori_loop(1, 16, step, 0)
    to_chip(z, (2, 1, 3))


def lane_iota(shape):
    return lax.broadcasted_iota(jnp.int32, shape, len(shape) - 1)


def body(
    x_hbm, pairs_hbm, observed_ref, kernel_ref, maps_ref, out_ref,
    x_raw, x_wide, x_ref, recv_a, send_b, recv_c, stage_b, stage_g, gram_m, onehot,
    stage_f, send_f, recv_f, send_g, recv_g, s_ref, send_i, recv_i, send_k, recv_k,
    obs_v, obs_rest, obs_rows, kern_v, maps_v, pairs_ref,
    local_sems, sems, ring_sems,
):
    zh = lax.axis_index("seg_0")
    far = zh * 32 + lax.axis_index("sta_0") * 4 + lax.axis_index("sta_1")
    near = lax.axis_index("seg_1") * 2 + lax.axis_index("seg_2")
    seg = zh * 8 + near

    load_x = pltpu.make_async_copy(x_hbm, x_raw, local_sems.at[0])
    load_pairs = pltpu.make_async_copy(pairs_hbm, pairs_ref, local_sems.at[1])
    loads = [
        pltpu.make_async_copy(observed_ref.at[seg], obs_v, local_sems.at[2]),
        pltpu.make_async_copy(observed_ref.at[16], obs_rest, local_sems.at[3]),
        pltpu.make_async_copy(kernel_ref, kern_v, local_sems.at[4]),
        pltpu.make_async_copy(maps_ref, maps_v, local_sems.at[5]),
    ]
    barrier = pltpu.get_barrier_semaphore()

    z, y = far // 4, far % 4

    def beside(dz, dy):
        return far_id(lax.rem(z + dz + 16, 16) * 4 + lax.rem(y + dy, 4))

    def greet(semaphore, device):
        pl.semaphore_signal(
            semaphore, inc=1, device_id=device, device_id_type=pl.DeviceIdType.MESH
        )

    load_x.start()
    for i in range(1, NEAR):
        greet(barrier, near_id(lax.rem(near + i, NEAR)))
    for dy in (1, 2, 3):
        greet(barrier, beside(0, dy))
    for dz in (1, -1):
        greet(barrier, beside(dz, 0))
    load_pairs.start()
    for load in loads:
        load.start()
    pl.semaphore_wait(barrier, NEAR - 1 + 5)
    for dz in (1, -1):
        greet(ring_sems.at[0], beside(dz, 0))
    load_x.wait()
    for i in range(24):
        x_wide[2 * i : 2 * i + 2, :] = x_raw[i // 4, i % 4].astype(F32)
    x_ref[...] = x_wide[...].astype(BF16)

    send_near(
        near,
        lambda peer: x_ref.at[:, pl.ds(pl.multiple_of(peer * 128, 128), 128)],
        lambda peer: recv_a.at[peer],
        sems, 0,
    )
    recv_a[near] = x_ref[:, pl.ds(pl.multiple_of(near * 128, 128), 128)]

    for step, distance in enumerate((1, 2, 4)):
        if step > 0:
            greet(ring_sems.at[step], beside(distance, 0))
            greet(ring_sems.at[step], beside(-distance, 0))
        pl.semaphore_wait(ring_sems.at[step], 2)
    greet(ring_sems.at[3], beside(-1, 0))
    pl.semaphore_wait(ring_sems.at[3], 1)
    load_pairs.wait()
    lane = lane_iota((1, 128))
    for end in range(2):
        row = jnp.zeros((1, 128), F32)
        for slot in range(17):
            row = jnp.where(lane == slot, pairs_ref[end, slot].astype(F32), row)
        stage_b[pl.ds(6 + end, FAR, stride=8), :] = jnp.broadcast_to(row, (FAR, 128))
    landed(recv_a.at[pl.ds(0, NEAR - 1)], sems.at[1])

    for pair in range(3):
        rows = []
        for a in (2 * pair, 2 * pair + 1):
            for m in range(NEAR):
                rows.append(recv_a[m].astype(F32)[8 * a : 8 * a + 8])
        turned = jnp.concatenate(rows, axis=0).T
        for fi in range(2):
            stage_b[pl.ds(3 * fi + pair, FAR, stride=8), :] = turned[64 * fi : 64 * fi + 64]
    send_b[...] = stage_b[...].reshape(FAR, 8, 128).astype(BF16)
    send_far(far, lambda peer: send_b.at[peer], lambda peer: recv_c.at[peer], sems, 2, True)
    recv_c[far] = send_b[far]
    for load in loads:
        load.wait()
    for a in range(STA_DEV):
        obs_rows[6 * a : 6 * a + 6, :] = obs_v[a]
    for j in range(4):
        pair = jnp.minimum(4 * seg + j, 35)
        obs_rows[36 + j : 37 + j, :] = obs_rest[pair // 6, pl.ds(pair % 6, 1), :]
    landed(recv_a.at[pl.ds(0, NEAR - 1)], sems.at[0])
    landed(recv_c.at[pl.ds(0, FAR - 1)], sems.at[3])
    stage_b[...] = recv_c[...].astype(F32).reshape(FAR * 8, 128)

    lane32 = lane_iota((32, 128))
    for fi in range(2):
        stations = []
        for pair in range(3):
            both = stage_b[pl.ds(3 * fi + pair, FAR, stride=8), :]
            low, high = both[0:32], both[32:64]
            stations.append(jnp.where(lane32 < 64, low, pltpu.roll(high, 64, 1)))
            stations.append(jnp.where(lane32 < 64, pltpu.roll(low, 64, 1), high))
        stations += [jnp.zeros((32, 128), F32)] * 2
        plain = jnp.concatenate(stations, axis=0)
        even = lax.rem(lane_iota((256, 128)), 2) == 0
        turned = jnp.where(even, pltpu.roll(plain, 127, 1), -pltpu.roll(plain, 1, 1))
        right = plain.astype(BF16)
        for c, left in enumerate((right, turned.astype(BF16))):
            gram = lax.dot_general(right, left, NT, preferred_element_type=F32)
            for i in range(8):
                at = PITCH * (8 * (2 * fi + c) + i)
                stage_g[0, at : at + 32, :] = gram[32 * i : 32 * i + 32, 0:128]
                stage_g[1, at : at + 32, :] = gram[32 * i : 32 * i + 32, 128:256]

    for tile in range(8):
        for half in range(2):
            pieces = [
                stage_g[half, pl.ds(4 * tile + i, 32, stride=PITCH), :] for i in range(4)
            ]
            for a in range(4 * half, min(4 * half + 4, STA_DEV)):
                kept = None
                for i, piece in enumerate(pieces):
                    shift = 32 * ((i - a) % 4)
                    piece = pltpu.roll(piece, shift, 1) if shift else piece
                    kept = piece if kept is None else jnp.where(lane32 >= 32 * i, piece, kept)
                gram_m[32 * a : 32 * a + 32, 128 * tile : 128 * tile + 128] = kept.astype(BF16)
    gram_m[192:256, :] = jnp.zeros((64, 1024), BF16)

    first = stage_b[pl.ds(6, FAR, stride=8), :]
    second = stage_b[pl.ds(7, FAR, stride=8), :]
    key = (second * 32.0 + first).astype(jnp.int32)
    row64 = lax.broadcasted_iota(jnp.int32, (FAR, 128), 0)
    main_key = jnp.where(row64 < 32, key, pltpu.roll(key, 120, 1))
    lane1024 = lane_iota((FAR, 1024))
    for m in range(NEAR + 1):
        column = key[:, 16:17] if m == NEAR else main_key[:, m : m + 1]
        hit = jnp.where(lane1024 == column, 1.0, 0.0)
        onehot[64 * m : 64 * m + 64, :] = hit.astype(BF16)
    slots = lax.dot_general(onehot[...], gram_m[...], NT, preferred_element_type=F32)
    slots = slots.astype(BF16)
    kept = jnp.dot(slots[0:512], maps_v[0], preferred_element_type=F32)
    for m in range(NEAR):
        stage_f[pl.ds(m, FAR, stride=16), :] = kept[64 * m : 64 * m + 64]
    rest = slots[512:576]
    upper = lax.broadcasted_iota(jnp.int32, (FAR, 256), 0) < 32
    rest_low = jnp.where(upper, rest, jnp.zeros_like(rest))
    rest_high = jnp.where(upper, jnp.zeros_like(rest), rest)
    for h in range(2):
        tail = jnp.dot(rest_low, maps_v[5 + h], preferred_element_type=F32)
        if h == 0:
            tail = tail + jnp.dot(rest_high, maps_v[7], preferred_element_type=F32)
        for i in range(4):
            at = 64 * (4 * h + i)
            tail = tail + jnp.dot(
                slots[at : at + 64], maps_v[1 + i], preferred_element_type=F32
            )
        stage_f[pl.ds(8 + h, FAR, stride=16), :] = tail
    send_f[...] = stage_f[...].astype(BF16)

    def chunk16(ref):
        return lambda peer: ref.at[pl.ds(pl.multiple_of(peer * 16, 16), 10), :]

    send_far(far, chunk16(send_f), chunk16(recv_f), sems, 4, True)
    own = pl.ds(pl.multiple_of(far * 16, 16), 16)
    recv_f[own, :] = send_f[own, :]
    landed(send_b.at[pl.ds(0, FAR - 1)], sems.at[2])
    landed(recv_f.at[pl.ds(0, 10 * (FAR - 1))], sems.at[5])
    stage_f[...] = recv_f[...].astype(F32)
    lane16 = lane_iota((16, 128))
    tails = [stage_f[pl.ds(8 + h, FAR, stride=16), :] for h in range(2)]
    for m in range(NEAR):
        send_g[m, 0:64, :] = stage_f[pl.ds(m, FAR, stride=16), :].astype(BF16)
        packed = None
        for i in range(4):
            piece = tails[m // 4][16 * i : 16 * i + 16]
            shift = 32 * ((i - m) % 4)
            piece = pltpu.roll(piece, shift, 1) if shift else piece
            packed = piece if packed is None else jnp.where(lane16 >= 32 * i, piece, packed)
        send_g[m, 64:80, :] = packed.astype(BF16)
    send_near(near, lambda peer: send_g.at[peer], lambda peer: recv_g.at[peer], sems, 6)
    recv_g[near] = send_g[near]
    landed(send_f.at[pl.ds(0, 10 * (FAR - 1))], sems.at[4])
    landed(recv_g.at[pl.ds(0, NEAR - 1)], sems.at[7])

    tail_rows = []
    for m in range(NEAR):
        blocks = recv_g[m, 64:80, :].astype(F32)
        for i in range(4):
            shift = 32 * ((m - i) % 4)
            tail_rows.append(pltpu.roll(blocks, shift, 1) if shift else blocks)
    lane128 = lane_iota((128, 128))
    tail = None
    for xt in range(4):
        both = jnp.concatenate(tail_rows[4 * xt : 4 * xt + 4] + tail_rows[4 * xt + 16 : 4 * xt + 20])
        tail = both if tail is None else jnp.where(lane128 >= 32 * xt, both, tail)
    tail = tail.T
    for xt in range(4):
        lanes = slice(128 * xt, 128 * xt + 128)
        square = jnp.concatenate(
            [recv_g[xt, 0:64, :].astype(F32), recv_g[4 + xt, 0:64, :].astype(F32)], axis=0
        ).T
        for fc in range(4):
            s_ref[fc, 0:32, lanes] = square[32 * fc : 32 * fc + 32]
            s_ref[fc, 32:40, lanes] = tail[32 * xt + 8 * fc : 32 * xt + 8 * fc + 8]
    lags = jnp.zeros((40, LAGS), F32)
    for fc in range(4):
        lags = lags + jnp.dot(s_ref[fc].astype(BF16), kern_v[fc], preferred_element_type=F32)

    def floor_of(slot):
        p, q = pairs_ref[0, slot], pairs_ref[1, slot]
        return jnp.where(p < 0, 99, jnp.where(p != q, -99, 0))

    row = lax.broadcasted_iota(jnp.int32, (40, LAGS), 0)
    pair = jnp.where(row < 36, row, jnp.minimum(row - 36 + 4 * seg, 35))
    floor = jnp.where(row < 36, floor_of(seg), jnp.where(seg < 9, floor_of(16), 99))
    keep = pair - 7 * sixths(pair) > floor
    value = jnp.tanh(SCALE * lags - obs_rows[...])
    residual = jnp.where(keep, value, 0.0).astype(BF16)

    to = lax.broadcasted_iota(jnp.int32, (16, 40), 0)
    of = lane_iota((16, 40))
    first_of = sixths(of)
    main = of < 36
    picked = (to < 6) & main & (first_of == to)
    picked = picked | ((to >= 6) & (to < 12) & main & (of - 6 * first_of == to - 6))
    picked = picked | ((of >= 36) & (of - 36 == to - 12))
    picked = jnp.where(picked, 1.0, 0.0).astype(BF16)
    for fi in range(2):
        gamma = [
            SCALE * lax.dot_general(residual, kern_v[2 * fi + c], NT, preferred_element_type=F32)
            for c in range(2)
        ]
        s0, s1 = s_ref[2 * fi], s_ref[2 * fi + 1]
        common = gamma[0] * s0 + gamma[1] * s1
        twist = gamma[1] * s0 - gamma[0] * s1
        for ct, term in enumerate((common, twist)):
            block = sum(
                jnp.dot(picked, third, preferred_element_type=F32) for third in thirds(term)
            )
            for xt in range(4):
                send_i[2 * xt + fi, 16 * ct : 16 * ct + 16, :] = block[:, 128 * xt : 128 * xt + 128]
    send_near(near, lambda peer: send_i.at[peer], lambda peer: recv_i.at[peer], sems, 8)
    recv_i[near] = send_i[near]

    lane = lane_iota((1, 128))
    source = lax.shift_right_logical(lane, 4)
    t = lane - 16 * source
    p_main = jnp.full((1, 128), -1, jnp.int32)
    q_main = p_main
    for m in range(NEAR):
        p_main = jnp.where(source == m, pairs_ref[0, zh * 8 + m], p_main)
        q_main = jnp.where(source == m, pairs_ref[1, zh * 8 + m], q_main)
    pair = jnp.clip(32 * zh + 4 * source + t - 12, 0, 35)
    valid = 32 * zh + 4 * source + t - 12 < 36
    a_rest = sixths(pair)
    plus = jnp.where(
        t < 6, 8 * p_main + t,
        jnp.where((t >= 12) & valid, 8 * pairs_ref[0, 16] + a_rest, -1),
    )
    minus = jnp.where(
        (t >= 6) & (t < 12), 8 * q_main + t - 6,
        jnp.where((t >= 12) & valid, 8 * pairs_ref[1, 16] + pair - 6 * a_rest, -1),
    )
    station = lax.broadcasted_iota(jnp.int32, (256, 128), 0)
    plus = jnp.where(station == plus, 1.0, 0.0)
    minus = jnp.where(station == minus, 1.0, 0.0)
    choose = ((plus + minus).astype(BF16), (plus - minus).astype(BF16))
    landed(send_g.at[pl.ds(0, NEAR - 1)], sems.at[6])
    landed(recv_i.at[pl.ds(0, NEAR - 1)], sems.at[9])
    sums = []
    for ct in range(2):
        terms = recv_i[:, 16 * ct : 16 * ct + 16, :].reshape(128, 128)
        sums.append(
            sum(jnp.dot(choose[ct], third, preferred_element_type=F32) for third in thirds(terms))
        )
    lane256 = lane_iota((256, 128))
    send_k[0:256, :] = jnp.where(lane256 < 64, sums[0], pltpu.roll(sums[1], 64, 1))
    send_k[256:512, :] = jnp.where(lane256 < 64, pltpu.roll(sums[0], 64, 1), sums[1])

    def chunk8(ref):
        return lambda peer: ref.at[pl.ds(pl.multiple_of(peer * 8, 8), STA_DEV), :]

    send_far(far, chunk8(send_k), chunk8(recv_k), sems, 10, True)
    own = pl.ds(pl.multiple_of(far * 8, 8), 8)
    recv_k[own, :] = send_k[own, :]
    landed(send_i.at[pl.ds(0, NEAR - 1)], sems.at[8])
    landed(recv_k.at[pl.ds(0, STA_DEV * (FAR - 1))], sems.at[11])
    total = recv_k[0:8, :]
    for k in range(1, FAR):
        total = total + recv_k[8 * k : 8 * k + 8, :]
    out_ref[:, 0, :] = total[0:STA_DEV, 0:64]
    out_ref[:, 1, :] = total[0:STA_DEV, 64:128]
    landed(send_k.at[pl.ds(0, STA_DEV * (FAR - 1))], sems.at[10])


def on_device(spectra, observed, pair_table):
    vmem = pl.BlockSpec(memory_space=pltpu.VMEM)
    hbm = pl.BlockSpec(memory_space=pl.ANY)
    return pl.pallas_call(
        body,
        out_shape=pltpu.VMEM((STA_DEV, 2, 64), F32),
        in_specs=[hbm] * 5,
        out_specs=vmem,
        scratch_shapes=[
            pltpu.VMEM((6, 4, 2, 1024), BF16),
            pltpu.VMEM((48, 1024), F32),
            pltpu.VMEM((48, 1024), BF16),
            pltpu.VMEM((8, 48, 128), BF16),
            pltpu.VMEM((64, 8, 128), BF16),
            pltpu.VMEM((64, 8, 128), BF16),
            pltpu.VMEM((512, 128), F32),
            pltpu.VMEM((2, 32 * PITCH, 128), F32),
            pltpu.VMEM((256, 1024), BF16),
            pltpu.VMEM((576, 1024), BF16),
            pltpu.VMEM((1024, 128), F32),
            pltpu.VMEM((1024, 128), BF16),
            pltpu.VMEM((1024, 128), BF16),
            pltpu.VMEM((8, 80, 128), BF16),
            pltpu.VMEM((8, 80, 128), BF16),
            pltpu.VMEM((4, 40, 512), F32),
            pltpu.VMEM((8, 32, 128), F32),
            pltpu.VMEM((8, 32, 128), F32),
            pltpu.VMEM((512, 128), F32),
            pltpu.VMEM((512, 128), F32),
            pltpu.VMEM((6, 6, 512), F32),
            pltpu.VMEM((6, 6, 512), F32),
            pltpu.VMEM((40, 512), F32),
            pltpu.VMEM((4, 512, 512), BF16),
            pltpu.VMEM((8, 256, 128), BF16),
            pltpu.SMEM((2, 17), jnp.int32),
            pltpu.SemaphoreType.DMA((6,)),
            pltpu.SemaphoreType.DMA((12,)),
            pltpu.SemaphoreType.REGULAR((4,)),
        ],
        compiler_params=pltpu.CompilerParams(collective_id=0, has_side_effects=True),
    )(spectra, pair_table.T, observed, lag_kernel(), lane_maps())


def solution(mesh):
    torus = Mesh(mesh.devices.reshape(8, 4, 2, 4, 2), ("sta_0", "sta_1", "seg_0", "seg_1", "seg_2"))
    in_specs = (P(STA, SEG, None, None), P(STA, None, None, None), P(STA, None))
    out_specs = P(STA, None, SEG)
    return jax.shard_map(
        on_device, mesh=torus, in_specs=in_specs, out_specs=out_specs, check_vma=False
    )
```
